32 devices in a mesh: graph: 8 (over z, y), row: 4 (over x, core).
Axes of the slice: x: 2, y: 2, z: 4, core: 2. Of those that a mesh axis runs over, the one named last changes fastest.
Arguments:
- tiles: bfloat16 [2048, 256, 256], P(('graph', 'row')), parts along dimension 0, may hold values from -0.25 to 0.25
- tile_rows: int32 [2048], P(('graph', 'row')), parts along dimension 0, may hold values from 0 to 15
- tile_cols: int32 [2048], P(('graph', 'row')), parts along dimension 0, may hold values from 0 to 63, as said below
- tile_count: int32 [32], P(('graph', 'row')), parts along dimension 0, may hold values from 8 to 64, as said below
- seeds: float32 [32, 131072], P(None, ('graph', 'row')), parts along dimension 1, may hold values from -6 to 6
- decay: float32 [32], replicated, may hold values from 0.8 to 1
Outputs:
- scores: float32 [32, 131072], P(None, ('graph', 'row')), parts along dimension 1
The draws below stay inside these ranges and needn't reach their ends.
There are 8 independent parts, one for each index of `graph`. The reference program is written for one: setup_inputs(seed, part) draws one part's arguments, and reference() takes and returns one part's arrays. A program takes and returns all parts, laid end to end along the dimension named above; an argument that names none is the same for every part. Nothing has to cross between parts.
Inputs may be any that keep to these rules, and one draw needn't show every extreme that they name: `tile_cols`: among the slots of one row panel, the tile columns that fall in the 16 tile rows of any one panel take at most 4 distinct values; in every draw the live slots of some panel take exactly 4 distinct tile columns of some one panel. Only the first tile_count slots of a panel are live; in every draw one panel has all 64 slots live.
All inputs are finite; a program needn't handle non-finite values.
Results may differ from the reference program's by a relative error of at most 0.0027.
Values may be sent and summed in bfloat16 or wider, within the bound.
A program may use at most 64 MiB of HBM per device.

```python
import jax
import jax.numpy as jnp
from jax import lax

TILE = 256
SEEDS = 32
BLK_DEV = 16
TILES_DEV = 64
NEED = 4
ITERS = 3
NBLK = 64
ORDER = 16384
TILES = 256
N_ROW = 4


def draw_tile_rows(key, part):
    return jax.random.randint(jax.random.fold_in(key, 11), (N_ROW * TILES_DEV,), 0, BLK_DEV).astype(jnp.int32)


def fullest_panel(key):
    return jax.random.randint(jax.random.fold_in(key, 14), (), 0, N_ROW)


def draw_tile_cols(key, part):
    pair_keys = jax.random.split(jax.random.fold_in(key, 21), N_ROW * N_ROW)
    choices = jax.vmap(lambda one: jax.random.permutation(one, BLK_DEV)[:NEED])(pair_keys)
    choices = choices.reshape(N_ROW, N_ROW, NEED).astype(jnp.int32)
    owning_panels = jax.random.randint(jax.random.fold_in(key, 22), (N_ROW, TILES_DEV), 0, N_ROW)
    picks = jax.random.randint(jax.random.fold_in(key, 23), (N_ROW, TILES_DEV), 0, NEED)
    fullest = fullest_panel(key)
    chosen_owner = jax.random.randint(jax.random.fold_in(key, 24), (), 0, N_ROW)
    panels = jnp.arange(N_ROW, dtype=jnp.int32)[:, None]
    slots = jnp.arange(TILES_DEV, dtype=jnp.int32)[None, :]
    forced = (panels == fullest) & (slots < NEED)
    owning_panels = jnp.where(forced, chosen_owner, owning_panels).astype(jnp.int32)
    picks = jnp.where(forced, slots, picks).astype(jnp.int32)
    panel_full = jnp.broadcast_to(panels, (N_ROW, TILES_DEV))
    local = choices[panel_full, owning_panels, picks]
    return (owning_panels * BLK_DEV + local).reshape(N_ROW * TILES_DEV).astype(jnp.int32)


def draw_tile_count(key, part):
    lower = max(TILES_DEV // 8, 1)
    base = jax.random.randint(jax.random.fold_in(key, 13), (N_ROW,), lower, TILES_DEV // 2 + 1)
    fullest = fullest_panel(key)
    panels = jnp.arange(N_ROW, dtype=jnp.int32)
    return jnp.where(panels == fullest, TILES_DEV, base).astype(jnp.int32)


def block_scale(key, extent, pieces, low, largest):
    def one(axis_at, parts):
        draws = jax.random.uniform(jax.random.fold_in(jax.random.fold_in(key, 6), axis_at), (parts,), jnp.float32, low / len(pieces), largest / len(pieces))
        return jnp.repeat(jnp.exp(draws), extent[axis_at] // parts).reshape((-1,) + (1,) * (len(extent) - axis_at - 1))

    gain = one(*pieces[0])
    for cut in pieces[1:]:
        gain = gain * one(*cut)
    return gain


def normal_values(own_key, extent, spread, limit, cuts=(), kind=jnp.bfloat16):
    entries = jax.random.normal(own_key, extent, jnp.float32) * spread
    if len(cuts) > 0:
        entries = block_scale(own_key, extent, cuts, -0.22, 0.18) * entries
    return jnp.clip(entries, min=-limit, max=limit).astype(kind)


def setup_inputs(seed: int = 0, part: int = 0) -> dict:
    splits = jax.random.split(jax.random.key(seed), 7)
    part_splits = jax.random.split(jax.random.fold_in(splits[6], part), 7)
    return {
        "tiles": normal_values(part_splits[0], (TILES, TILE, TILE), (TILE * 2) ** -0.5, 0.25, ((0, 4),)),
        "tile_rows": draw_tile_rows(jax.random.fold_in(jax.random.fold_in(splits[6], part), 71), part),
        "tile_cols": draw_tile_cols(jax.random.fold_in(jax.random.fold_in(splits[6], part), 71), part),
        "tile_count": draw_tile_count(jax.random.fold_in(jax.random.fold_in(splits[6], part), 71), part),
        "seeds": normal_values(part_splits[4], (SEEDS, ORDER), 1.0, 6.0, ((1, 4),), jnp.float32),
        "decay": jnp.clip(jax.random.uniform(splits[5], (SEEDS,), jnp.float32, 0.8, 1.0), 0.8, 1.0),
    }


def reference(tiles, tile_rows, tile_cols, tile_count, seeds, decay):
    slot_index = jnp.arange(N_ROW * TILES_DEV, dtype=jnp.int32)
    panel = slot_index // TILES_DEV
    active_flag = slot_index % TILES_DEV < tile_count[panel]
    target = (panel * BLK_DEV + tile_rows).astype(jnp.int32)
    weight = active_flag.astype(jnp.float32)
    tiles_wide = tiles.astype(jnp.float32)
    iterate = seeds
    for step in range(ITERS):
        rounded = iterate.astype(jnp.bfloat16)
        blocks = rounded.reshape(SEEDS, NBLK, TILE)
        picked = jnp.take(blocks, tile_cols, axis=1).astype(jnp.float32)
        block_products = jnp.einsum('trc,stc->tsr', tiles_wide, picked, precision=lax.Precision.HIGHEST)
        block_products = block_products * weight[:, None, None]
        reduced_sum = jax.ops.segment_sum(block_products, target, num_segments=NBLK)
        reduced_sum = jnp.transpose(reduced_sum, (1, 0, 2)).reshape(SEEDS, NBLK * TILE)
        iterate = decay[:, None] * reduced_sum + seeds
    norm_value = jnp.sqrt(lax.optimization_barrier(jnp.mean(iterate * iterate, axis=1, keepdims=True)) + 1e-06)
    return iterate / norm_value
```

```python
import functools

import jax
import jax.numpy as jnp
from jax import lax
from jax.experimental import pallas as pl
from jax.experimental.pallas import tpu as pltpu
from jax.sharding import PartitionSpec as P

TILE = 256
NEED = 4
HALVES = 2
ITERS = 3
MESH = pl.DeviceIdType.MESH
LANES = 128
ROW_PERM, ROW_PLACE, ROW_KEEP, ROW_LAST, ROW_HAS = 0, 1, 2, 3, 4


def spread(ref, slots, square):
    wide = jnp.concatenate(
        [ref[...], jnp.zeros((1, square - slots), jnp.int32)], axis=1
    ) if square > slots else ref[...]
    return jnp.broadcast_to(wide, (square, square))


def fill_wanted(cols_ref, count, wanted, slots, blk):
    width = wanted.shape[1]
    square = max(LANES, slots)
    lane = lax.broadcasted_iota(jnp.int32, (square, square), 1)
    col_row = jnp.where((lane < count) & (lane < slots), spread(cols_ref, slots, square), -1)
    col_t = jnp.transpose(col_row)[:slots, :1]
    lane_c = lax.broadcasted_iota(jnp.int32, (slots, width), 1)
    hit = (col_t == lane_c).astype(jnp.int32)
    lane_w = lax.broadcasted_iota(jnp.int32, (8, width), 1)
    local = lane_w % blk
    present = jnp.broadcast_to(jnp.max(hit, axis=0, keepdims=True), (8, width))

    def scan(value):
        step = 1
        while step < blk:
            value = value + jnp.where(local >= step, pltpu.roll(value, step, 1), 0)
            step *= 2
        return value

    rank = scan(present) - 1
    which = lax.broadcasted_iota(jnp.int32, (8, width), 0)
    chosen = (present > 0) & (rank == which)
    wanted[...] = scan(jnp.where(chosen, local, 0))
    weight = (lane_w // blk) * NEED + rank
    return hit, weight


def fill_own(rows_ref, count, own_table, hit, weight, slots, blk):
    width = hit.shape[1]
    square = max(LANES, slots)
    lane = lax.broadcasted_iota(jnp.int32, (square, square), 1)
    sub = lax.broadcasted_iota(jnp.int32, (square, square), 0)
    key_row = jnp.where(lane < count, spread(rows_ref, slots, square), blk)
    key_row = jnp.where(lane < slots, key_row, blk + 1)
    key_c = jnp.transpose(key_row)[:slots, :]
    key_r = key_row[:slots, :]
    place_col = jnp.sum(hit * weight[:1, :], axis=1, keepdims=True)
    place_col = jnp.clip(place_col, 0, (width // blk) * NEED - 1)
    lane_s, sub_s = lane[:slots, :], sub[:slots, :]
    before = (key_r < key_c) | ((key_r == key_c) & (lane_s < sub_s))
    position = jnp.sum((before & (lane_s < slots)).astype(jnp.int32), axis=1, keepdims=True)
    at = position == lane_s
    perm = jnp.sum(jnp.where(at, sub_s, 0), axis=0, keepdims=True)
    place = jnp.sum(jnp.where(at, place_col, 0), axis=0, keepdims=True)
    key_sorted = jnp.sum(jnp.where(at, key_c, 0), axis=0, keepdims=True)
    previous = jnp.sum(jnp.where(position + 1 == lane_s, key_c, 0), axis=0, keepdims=True)
    keep = ((key_sorted == previous) & (lane_s[:1, :] > 0)).astype(jnp.int32)
    last = jnp.sum((key_c <= lane_s).astype(jnp.int32), axis=0, keepdims=True) - 1
    has = jnp.max((key_c == lane_s).astype(jnp.int32), axis=0, keepdims=True)
    own_table[...] = jnp.zeros(own_table.shape, jnp.int32)
    own_table[ROW_PERM:ROW_PERM + 1, :] = perm
    own_table[ROW_PLACE:ROW_PLACE + 1, :] = place
    own_table[ROW_KEEP:ROW_KEEP + 1, :] = keep
    own_table[ROW_LAST:ROW_LAST + 1, :] = jnp.maximum(last, 0)
    own_table[ROW_HAS:ROW_HAS + 1, :] = has


def kernel(
    panels, slots, blk, seed_count, chunks, unroll, halves,
    count_ref, cols_hbm, rows_hbm, decay_hbm, seeds_hbm, tiles_hbm,
    out_ref,
    tiles, turned, seeds_ref, current, outgoing, partial, own_table, wanted, squares,
    rows_ref, cols_ref, decay_ref, own_s, wanted_s,
    tile_sem, seed_sem, small_sem, table_sem,
    want_send, want_recv, send_sem, recv_sem, norm_send, norm_recv,
    *arrivals,
):
    me = lax.axis_index("row")
    cores = 2 if panels % 2 == 0 else 1
    chip, core = me // cores, me % cores
    groups = panels // cores
    rows = seed_count // halves
    peers = [
        lax.rem(chip + d, groups) * cores + e
        for d in range(groups - 1, 0, -1) for e in range(cores)
    ] + [chip * cores + lax.rem(core + e, cores) for e in range(1, cores)]

    small = [
        pltpu.make_async_copy(src, dst, small_sem.at[n])
        for n, (src, dst) in enumerate([
            (cols_hbm, cols_ref), (rows_hbm, rows_ref), (decay_hbm, decay_ref),
        ])
    ]
    for copy in small:
        copy.start()
    barrier = pltpu.get_barrier_semaphore()
    for peer in peers:
        pl.semaphore_signal(barrier, inc=1, device_id={"row": peer}, device_id_type=MESH)

    seed_load = pltpu.make_async_copy(seeds_hbm, seeds_ref, seed_sem.at[0])
    seed_load.start()
    per = slots // chunks

    def load(c):
        return pltpu.make_async_copy(
            tiles_hbm.at[pl.ds(c * per, per)], tiles.at[pl.ds(c * per, per)], tile_sem.at[c]
        )

    for c in range(chunks):
        load(c).start()

    small[0].wait()
    count = count_ref[0]
    hit, weight = fill_wanted(cols_ref, count, wanted, slots, blk)
    pl.semaphore_wait(barrier, panels - 1)

    def ask(n, peer, source):
        return pltpu.make_async_remote_copy(
            src_ref=wanted, dst_ref=wanted_s.at[source],
            send_sem=want_send.at[n], recv_sem=want_recv.at[source],
            device_id={"row": peer}, device_id_type=MESH,
        )

    for n, peer in enumerate(peers):
        ask(n, peer, me).start()
    want_copy = pltpu.make_async_copy(wanted, wanted_s.at[me], table_sem.at[1])
    want_copy.start()
    small[1].wait()
    fill_own(rows_ref, count, own_table, hit, weight, slots, blk)
    own_copy = pltpu.make_async_copy(own_table, own_s, table_sem.at[0])
    own_copy.start()
    small[2].wait()

    seed_load.wait()
    for h in range(halves):
        for b in range(blk):
            current[h, b] = seeds_ref[
                h * rows:(h + 1) * rows, b * TILE:(b + 1) * TILE
            ].astype(jnp.bfloat16)
    diagonal = lax.broadcasted_iota(jnp.int32, (seed_count, seed_count), 0) == (
        lax.broadcasted_iota(jnp.int32, (seed_count, seed_count), 1)
    )
    decay = jnp.sum(
        jnp.where(diagonal, jnp.broadcast_to(decay_ref[...], diagonal.shape), 0.0),
        axis=1, keepdims=True,
    )

    for n, peer in enumerate(peers):
        ask(n, peer, peer).wait_recv()
    want_copy.wait()

    def ship(it, h, n, peer, source):
        return pltpu.make_async_remote_copy(
            src_ref=outgoing.at[it, h, n],
            dst_ref=arrivals[it * halves + h].at[pl.ds(source * NEED, NEED)],
            send_sem=send_sem.at[it, h, n], recv_sem=recv_sem.at[it, h, source],
            device_id={"row": peer}, device_id_type=MESH,
        )

    def exchange(it, h):
        arrived = arrivals[it * halves + h]
        for n, peer in enumerate(peers):
            for k in range(NEED):
                outgoing[it, h, n, k] = current[h, wanted_s[peer, k, me * blk + blk - 1]]
            ship(it, h, n, peer, me).start()
        for k in range(NEED):
            arrived[me * NEED + k] = current[h, wanted_s[me, k, me * blk + blk - 1]]

    for h in range(halves):
        exchange(0, h)

    def turn(c, carry):
        load(c).wait()
        for i in range(per):
            turned[c * per + i] = jnp.transpose(tiles[c * per + i])
        return carry

    lax.fori_loop(0, chunks, turn, 0)
    own_copy.wait()

    totals = []
    for it in range(ITERS):
        for h in range(halves):
            arrived = arrivals[it * halves + h]
            for n, peer in enumerate(peers):
                ship(it, h, n, peer, peer).wait_recv()

            def some(group, acc):
                for u in range(unroll):
                    j = group * unroll + u
                    product = jnp.dot(
                        arrived[own_s[ROW_PLACE, j]], turned[own_s[ROW_PERM, j]],
                        preferred_element_type=jnp.float32,
                    )
                    acc = acc * own_s[ROW_KEEP, j].astype(jnp.float32) + product
                    partial[h, j] = acc
                return acc

            lax.fori_loop(0, slots // unroll, some, jnp.zeros((rows, TILE), jnp.float32))

            mine = slice(h * rows, (h + 1) * rows)
            total = jnp.zeros((rows, TILE), jnp.float32)
            for r in range(blk):
                summed = partial[h, own_s[ROW_LAST, r]] * own_s[ROW_HAS, r].astype(jnp.float32)
                value = decay[mine] * summed + seeds_ref[mine, r * TILE:(r + 1) * TILE]
                if it < ITERS - 1:
                    current[h, r] = value.astype(jnp.bfloat16)
                else:
                    out_ref[mine, r * TILE:(r + 1) * TILE] = value
                    total = total + value * value
            if it < ITERS - 1:
                exchange(it + 1, h)
            else:
                totals.append(jnp.sum(total, axis=1, keepdims=True))

    lane = lax.broadcasted_iota(jnp.int32, (8, LANES), 1)
    packed = jnp.zeros((8, LANES), jnp.float32)
    pieces = [t[i:i + 8] for t in totals for i in range(0, rows, 8)]
    for i, piece in enumerate(pieces):
        packed = jnp.where(lane == i, piece, packed)
    squares[me] = packed

    def share(n, peer, source):
        return pltpu.make_async_remote_copy(
            src_ref=squares.at[me], dst_ref=squares.at[source],
            send_sem=norm_send.at[n], recv_sem=norm_recv.at[source],
            device_id={"row": peer}, device_id_type=MESH,
        )

    for n, peer in enumerate(peers):
        share(n, peer, me).start()
    for n, peer in enumerate(peers):
        for it in range(ITERS):
            for h in range(halves):
                ship(it, h, n, peer, me).wait_send()
        ask(n, peer, me).wait_send()
    for n, peer in enumerate(peers):
        share(n, peer, peer).wait_recv()
    every = squares[0]
    for p in range(1, panels):
        every = every + squares[p]
    scale = 1.0 / jnp.sqrt(every / (panels * blk * TILE) + 1e-06)
    for i in range(len(pieces)):
        one = jnp.sum(jnp.where(lane == i, scale, 0.0), axis=1, keepdims=True)
        out_ref[i * 8:(i + 1) * 8, :] = out_ref[i * 8:(i + 1) * 8, :] * one
    for n, peer in enumerate(peers):
        share(n, peer, me).wait_send()


def per_device(tiles, tile_rows, tile_cols, tile_count, seeds, decay):
    slots = tiles.shape[0]
    seed_count = seeds.shape[0]
    blk = seeds.shape[1] // TILE
    panels = lax.axis_size("row")
    width = -(-panels * blk // LANES) * LANES
    square = max(LANES, slots)
    chunks = 8 if slots % 8 == 0 else 1
    unroll = 64 if slots % 64 == 0 else 1
    halves = HALVES if seed_count % (16 * HALVES) == 0 else 1
    rows = seed_count // halves
    peers = panels - 1
    vmem = pl.BlockSpec(memory_space=pltpu.VMEM)
    dma = pltpu.SemaphoreType.DMA
    return pl.pallas_call(
        functools.partial(kernel, panels, slots, blk, seed_count, chunks, unroll, halves),
        out_shape=jax.ShapeDtypeStruct(seeds.shape, jnp.float32),
        in_specs=[pl.BlockSpec(memory_space=pltpu.SMEM)] + [pl.BlockSpec(memory_space=pltpu.HBM)] * 5,
        out_specs=vmem,
        scratch_shapes=[
            pltpu.VMEM((slots, TILE, TILE), jnp.bfloat16),
            pltpu.VMEM((slots, TILE, TILE), jnp.bfloat16),
            pltpu.VMEM(seeds.shape, jnp.float32),
            pltpu.VMEM((halves, blk, rows, TILE), jnp.bfloat16),
            pltpu.VMEM((ITERS, halves, peers, NEED, rows, TILE), jnp.bfloat16),
            pltpu.VMEM((halves, slots, rows, TILE), jnp.float32),
            pltpu.VMEM((8, square), jnp.int32),
            pltpu.VMEM((8, width), jnp.int32),
            pltpu.VMEM((panels, 8, LANES), jnp.float32),
            pltpu.VMEM((1, slots), jnp.int32),
            pltpu.VMEM((1, slots), jnp.int32),
            pltpu.VMEM((1, seed_count), jnp.float32),
            pltpu.SMEM((8, square), jnp.int32),
            pltpu.SMEM((panels, 8, width), jnp.int32),
            dma((chunks,)), dma((1,)), dma((3,)), dma((2,)), dma((peers,)), dma((panels,)),
            dma((ITERS, halves, peers)), dma((ITERS, halves, panels)),
            dma((peers,)), dma((panels,)),
            *[
                pltpu.VMEM((panels * NEED, rows, TILE), jnp.bfloat16)
                for _ in range(ITERS * halves)
            ],
        ],
        compiler_params=pltpu.CompilerParams(
            collective_id=0, has_side_effects=True, vmem_limit_bytes=53 * 2**20
        ),
    )(tile_count, *[
        pltpu.with_memory_space_constraint(one, pltpu.HBM)
        for one in (
            tile_cols.reshape(1, slots), tile_rows.reshape(1, slots),
            decay.reshape(1, seed_count), seeds, tiles,
        )
    ])


def solution(mesh):
    in_specs = (
        P(("graph", "row"), None, None),
        P(("graph", "row")),
        P(("graph", "row")),
        P(("graph", "row")),
        P(None, ("graph", "row")),
        P(),
    )
    out_specs = P(None, ("graph", "row"))
    return jax.shard_map(
        per_device, mesh=mesh, in_specs=in_specs, out_specs=out_specs, check_vma=False
    )
```

```python
import functools

import jax
import jax.numpy as jnp
from jax import lax
from jax.experimental import pallas as pl
from jax.experimental.pallas import tpu as pltpu
from jax.sharding import PartitionSpec as P

TILE = 256
NEED = 4
HALVES = 2
PARTS = 2
ITERS = 3
MESH = pl.DeviceIdType.MESH
LANES = 128
ROW_PERM, ROW_PLACE, ROW_KEEP, ROW_LAST, ROW_HAS, ROW_COL = 0, 1, 2, 3, 4, 5


def spread(ref, slots, square):
    wide = jnp.concatenate(
        [ref[...], jnp.zeros((1, square - slots), jnp.int32)], axis=1
    ) if square > slots else ref[...]
    return jnp.broadcast_to(wide, (square, square))


def fill_wanted(cols_ref, count, wanted, slots, blk):
    width = wanted.shape[1]
    square = max(LANES, slots)
    lane = lax.broadcasted_iota(jnp.int32, (square, square), 1)
    col_row = jnp.where((lane < count) & (lane < slots), spread(cols_ref, slots, square), -1)
    col_t = jnp.transpose(col_row)[:slots, :1]
    lane_c = lax.broadcasted_iota(jnp.int32, (slots, width), 1)
    hit = (col_t == lane_c).astype(jnp.int32)
    lane_w = lax.broadcasted_iota(jnp.int32, (8, width), 1)
    local = lane_w % blk
    present = jnp.broadcast_to(jnp.max(hit, axis=0, keepdims=True), (8, width))

    def scan(value):
        step = 1
        while step < blk:
            value = value + jnp.where(local >= step, pltpu.roll(value, step, 1), 0)
            step *= 2
        return value

    rank = scan(present) - 1
    which = lax.broadcasted_iota(jnp.int32, (8, width), 0)
    chosen = (present > 0) & (rank == which)
    wanted[...] = scan(jnp.where(chosen, local, 0))
    weight = (lane_w // blk) * NEED + rank
    return hit, weight, col_t


def fill_own(rows_ref, count, own_table, hit, weight, col_t, slots, blk):
    width = hit.shape[1]
    square = max(LANES, slots)
    lane = lax.broadcasted_iota(jnp.int32, (square, square), 1)
    sub = lax.broadcasted_iota(jnp.int32, (square, square), 0)
    key_row = jnp.where(lane < count, spread(rows_ref, slots, square), blk)
    key_row = jnp.where(lane < slots, key_row, blk + 1)
    key_c = jnp.transpose(key_row)[:slots, :]
    key_r = key_row[:slots, :]
    place_col = jnp.sum(hit * weight[:1, :], axis=1, keepdims=True)
    place_col = jnp.clip(place_col, 0, (width // blk) * NEED - 1)
    lane_s, sub_s = lane[:slots, :], sub[:slots, :]
    before = (key_r < key_c) | ((key_r == key_c) & (lane_s < sub_s))
    position = jnp.sum((before & (lane_s < slots)).astype(jnp.int32), axis=1, keepdims=True)
    at = position == lane_s
    perm = jnp.sum(jnp.where(at, sub_s, 0), axis=0, keepdims=True)
    place = jnp.sum(jnp.where(at, place_col, 0), axis=0, keepdims=True)
    column = jnp.sum(jnp.where(at, jnp.clip(col_t, 0, width - 1), 0), axis=0, keepdims=True)
    key_sorted = jnp.sum(jnp.where(at, key_c, 0), axis=0, keepdims=True)
    previous = jnp.sum(jnp.where(position + 1 == lane_s, key_c, 0), axis=0, keepdims=True)
    keep = ((key_sorted == previous) & (lane_s[:1, :] > 0)).astype(jnp.int32)
    last = jnp.sum((key_c <= lane_s).astype(jnp.int32), axis=0, keepdims=True) - 1
    has = jnp.max((key_c == lane_s).astype(jnp.int32), axis=0, keepdims=True)
    own_table[...] = jnp.zeros(own_table.shape, jnp.int32)
    own_table[ROW_PERM:ROW_PERM + 1, :] = perm
    own_table[ROW_PLACE:ROW_PLACE + 1, :] = place
    own_table[ROW_KEEP:ROW_KEEP + 1, :] = keep
    own_table[ROW_LAST:ROW_LAST + 1, :] = jnp.maximum(last, 0)
    own_table[ROW_HAS:ROW_HAS + 1, :] = has
    own_table[ROW_COL:ROW_COL + 1, :] = column


def kernel(
    panels, slots, blk, seed_count, chunks, unroll, halves,
    count_ref, cols_hbm, rows_hbm, decay_hbm, seeds_hbm, tiles_hbm,
    out_ref,
    tiles, turned, seeds_ref, current, outgoing, partial, own_table, wanted, squares,
    rows_ref, cols_ref, decay_ref, own_s, wanted_s,
    tile_sem, seed_sem, small_sem, table_sem,
    want_send, want_recv, send_sem, recv_sem, norm_send, norm_recv,
    bulk_send, bulk_recv, pass_send, pass_recv, near_send, near_recv, whole,
    *arrivals,
):
    me = lax.axis_index("row")
    cores = 2 if panels % 2 == 0 else 1
    chip, core = me // cores, me % cores
    groups = panels // cores
    rows = seed_count // halves
    peers = [
        lax.rem(chip + d, groups) * cores + e
        for d in range(groups - 1, 0, -1) for e in range(cores)
    ] + [chip * cores + lax.rem(core + e, cores) for e in range(1, cores)]

    small = [
        pltpu.make_async_copy(src, dst, small_sem.at[n])
        for n, (src, dst) in enumerate([
            (cols_hbm, cols_ref), (rows_hbm, rows_ref), (decay_hbm, decay_ref),
        ])
    ]
    for copy in small:
        copy.start()
    barrier = pltpu.get_barrier_semaphore()
    for peer in peers:
        pl.semaphore_signal(barrier, inc=1, device_id={"row": peer}, device_id_type=MESH)

    seed_load = pltpu.make_async_copy(seeds_hbm, seeds_ref, seed_sem.at[0])
    seed_load.start()
    per = slots // chunks

    def load(c):
        return pltpu.make_async_copy(
            tiles_hbm.at[pl.ds(c * per, per)], tiles.at[pl.ds(c * per, per)], tile_sem.at[c]
        )

    for c in range(chunks):
        load(c).start(priority=1)

    small[0].wait()
    count = count_ref[0]
    hit, weight, col_t = fill_wanted(cols_ref, count, wanted, slots, blk)
    seed_load.wait()
    for b in range(blk):
        nodes = slice(b * TILE, (b + 1) * TILE)
        whole[me * blk + b] = seeds_ref[:rows, nodes].astype(jnp.bfloat16)
    pl.semaphore_wait(barrier, panels - 1)

    def ask(n, peer, source):
        return pltpu.make_async_remote_copy(
            src_ref=wanted, dst_ref=wanted_s.at[source],
            send_sem=want_send.at[n], recv_sem=want_recv.at[source],
            device_id={"row": peer}, device_id_type=MESH,
        )

    for n, peer in enumerate(peers):
        ask(n, peer, me).start()
    span = blk // PARTS
    partner = chip * cores + (cores - 1 - core)

    def block(source, part):
        return whole.at[pl.ds(source * blk + part * span, span)]

    def bulk(d, part, source):
        far = lax.rem(chip + d, groups) * cores + (cores - 1 - core)
        return pltpu.make_async_remote_copy(
            src_ref=block(source, part), dst_ref=block(source, part),
            send_sem=bulk_send.at[d - 1, part], recv_sem=bulk_recv.at[d - 1, part],
            device_id={"row": far}, device_id_type=MESH,
        )

    def hand(d, part, source):
        return pltpu.make_async_remote_copy(
            src_ref=block(source, part), dst_ref=block(source, part),
            send_sem=pass_send.at[d - 1, part], recv_sem=pass_recv.at[d - 1, part],
            device_id={"row": partner}, device_id_type=MESH,
        )

    def near(source):
        return pltpu.make_async_remote_copy(
            src_ref=whole.at[pl.ds(source * blk, blk)], dst_ref=whole.at[pl.ds(source * blk, blk)],
            send_sem=near_send.at[0], recv_sem=near_recv.at[0],
            device_id={"row": partner}, device_id_type=MESH,
        )

    def origin(d, index):
        return lax.rem(chip + groups - d, groups) * cores + index

    for part in range(PARTS):
        for d in range(1, groups):
            bulk(d, part, me).start()
    if cores > 1:
        near(me).start()
    want_copy = pltpu.make_async_copy(wanted, wanted_s.at[me], table_sem.at[1])
    want_copy.start()
    small[1].wait()
    fill_own(rows_ref, count, own_table, hit, weight, col_t, slots, blk)
    own_copy = pltpu.make_async_copy(own_table, own_s, table_sem.at[0])
    own_copy.start()
    small[2].wait()
    for h in range(1, halves):
        for b in range(blk):
            current[h, b] = seeds_ref[
                h * rows:(h + 1) * rows, b * TILE:(b + 1) * TILE
            ].astype(jnp.bfloat16)
    diagonal = lax.broadcasted_iota(jnp.int32, (seed_count, seed_count), 0) == (
        lax.broadcasted_iota(jnp.int32, (seed_count, seed_count), 1)
    )
    decay = jnp.sum(
        jnp.where(diagonal, jnp.broadcast_to(decay_ref[...], diagonal.shape), 0.0),
        axis=1, keepdims=True,
    )

    def turn(c, carry):
        load(c).wait()
        for i in range(per):
            turned[c * per + i] = jnp.transpose(tiles[c * per + i])
        return carry

    lax.fori_loop(0, chunks, turn, 0)
    for n, peer in enumerate(peers):
        ask(n, peer, peer).wait_recv()
    want_copy.wait()

    def ship(it, h, n, peer, source):
        return pltpu.make_async_remote_copy(
            src_ref=outgoing.at[it, h, n],
            dst_ref=arrivals[it * halves + h].at[pl.ds(source * NEED, NEED)],
            send_sem=send_sem.at[it, h, n], recv_sem=recv_sem.at[it, h, source],
            device_id={"row": peer}, device_id_type=MESH,
        )

    def exchange(it, h):
        arrived = arrivals[it * halves + h]
        for n, peer in enumerate(peers):
            for k in range(NEED):
                outgoing[it, h, n, k] = current[h, wanted_s[peer, k, me * blk + blk - 1]]
            ship(it, h, n, peer, me).start()
        for k in range(NEED):
            arrived[me * NEED + k] = current[h, wanted_s[me, k, me * blk + blk - 1]]

    for h in range(1, halves):
        exchange(0, h)
    for part in range(PARTS):
        for d in range(1, groups):
            source = origin(d, cores - 1 - core)
            bulk(d, part, source).wait_recv()
            if cores > 1:
                hand(d, part, source).start()

    own_copy.wait()

    totals = []
    for it in range(ITERS):
        for h in range(halves):
            first = it == 0 and h == 0
            arrived = whole if first else arrivals[it * halves + h]
            row_at = ROW_COL if first else ROW_PLACE
            if first and cores > 1:
                near(partner).wait_recv()
                for part in range(PARTS):
                    for d in range(1, groups):
                        hand(d, part, origin(d, core)).wait_recv()
            if not first:
                for n, peer in enumerate(peers):
                    ship(it, h, n, peer, peer).wait_recv()

            def some(group, acc):
                for u in range(unroll):
                    j = group * unroll + u
                    product = jnp.dot(
                        arrived[own_s[row_at, j]], turned[own_s[ROW_PERM, j]],
                        preferred_element_type=jnp.float32,
                    )
                    acc = acc * own_s[ROW_KEEP, j].astype(jnp.float32) + product
                    partial[h, j] = acc
                return acc

            lax.fori_loop(0, slots // unroll, some, jnp.zeros((rows, TILE), jnp.float32))

            mine = slice(h * rows, (h + 1) * rows)
            total = jnp.zeros((rows, TILE), jnp.float32)
            for r in range(blk):
                summed = partial[h, own_s[ROW_LAST, r]] * own_s[ROW_HAS, r].astype(jnp.float32)
                value = decay[mine] * summed + seeds_ref[mine, r * TILE:(r + 1) * TILE]
                if it < ITERS - 1:
                    current[h, r] = value.astype(jnp.bfloat16)
                else:
                    out_ref[mine, r * TILE:(r + 1) * TILE] = value
                    total = total + value * value
            if it < ITERS - 1:
                exchange(it + 1, h)
            else:
                totals.append(jnp.sum(total, axis=1, keepdims=True))

    lane = lax.broadcasted_iota(jnp.int32, (8, LANES), 1)
    packed = jnp.zeros((8, LANES), jnp.float32)
    pieces = [t[i:i + 8] for t in totals for i in range(0, rows, 8)]
    for i, piece in enumerate(pieces):
        packed = jnp.where(lane == i, piece, packed)
    squares[me] = packed

    def share(n, peer, source):
        return pltpu.make_async_remote_copy(
            src_ref=squares.at[me], dst_ref=squares.at[source],
            send_sem=norm_send.at[n], recv_sem=norm_recv.at[source],
            device_id={"row": peer}, device_id_type=MESH,
        )

    for n, peer in enumerate(peers):
        share(n, peer, me).start()
    for n, peer in enumerate(peers):
        for it in range(ITERS):
            for h in range(halves):
                if (it, h) != (0, 0):
                    ship(it, h, n, peer, me).wait_send()
        ask(n, peer, me).wait_send()
    for part in range(PARTS):
        for d in range(1, groups):
            bulk(d, part, me).wait_send()
            if cores > 1:
                hand(d, part, origin(d, cores - 1 - core)).wait_send()
    if cores > 1:
        near(me).wait_send()
    for n, peer in enumerate(peers):
        share(n, peer, peer).wait_recv()
    every = squares[0]
    for p in range(1, panels):
        every = every + squares[p]
    scale = 1.0 / jnp.sqrt(every / (panels * blk * TILE) + 1e-06)
    for i in range(len(pieces)):
        one = jnp.sum(jnp.where(lane == i, scale, 0.0), axis=1, keepdims=True)
        out_ref[i * 8:(i + 1) * 8, :] = out_ref[i * 8:(i + 1) * 8, :] * one
    for n, peer in enumerate(peers):
        share(n, peer, me).wait_send()


def per_device(tiles, tile_rows, tile_cols, tile_count, seeds, decay):
    slots = tiles.shape[0]
    seed_count = seeds.shape[0]
    blk = seeds.shape[1] // TILE
    panels = lax.axis_size("row")
    width = -(-panels * blk // LANES) * LANES
    square = max(LANES, slots)
    chunks = 8 if slots % 8 == 0 else 1
    unroll = 64 if slots % 64 == 0 else 1
    halves = HALVES if seed_count % (16 * HALVES) == 0 else 1
    rows = seed_count // halves
    peers = panels - 1
    far = max(panels // (2 if panels % 2 == 0 else 1) - 1, 1)
    vmem = pl.BlockSpec(memory_space=pltpu.VMEM)
    dma = pltpu.SemaphoreType.DMA
    return pl.pallas_call(
        functools.partial(kernel, panels, slots, blk, seed_count, chunks, unroll, halves),
        out_shape=jax.ShapeDtypeStruct(seeds.shape, jnp.float32),
        in_specs=[pl.BlockSpec(memory_space=pltpu.SMEM)] + [pl.BlockSpec(memory_space=pltpu.HBM)] * 5,
        out_specs=vmem,
        scratch_shapes=[
            pltpu.VMEM((slots, TILE, TILE), jnp.bfloat16),
            pltpu.VMEM((slots, TILE, TILE), jnp.bfloat16),
            pltpu.VMEM(seeds.shape, jnp.float32),
            pltpu.VMEM((halves, blk, rows, TILE), jnp.bfloat16),
            pltpu.VMEM((ITERS, halves, peers, NEED, rows, TILE), jnp.bfloat16),
            pltpu.VMEM((halves, slots, rows, TILE), jnp.float32),
            pltpu.VMEM((8, square), jnp.int32),
            pltpu.VMEM((8, width), jnp.int32),
            pltpu.VMEM((panels, 8, LANES), jnp.float32),
            pltpu.VMEM((1, slots), jnp.int32),
            pltpu.VMEM((1, slots), jnp.int32),
            pltpu.VMEM((1, seed_count), jnp.float32),
            pltpu.SMEM((8, square), jnp.int32),
            pltpu.SMEM((panels, 8, width), jnp.int32),
            dma((chunks,)), dma((1,)), dma((3,)), dma((2,)), dma((peers,)), dma((panels,)),
            dma((ITERS, halves, peers)), dma((ITERS, halves, panels)),
            dma((peers,)), dma((panels,)),
            dma((far, PARTS)), dma((far, PARTS)), dma((far, PARTS)), dma((far, PARTS)),
            dma((1,)), dma((1,)),
            pltpu.VMEM((panels * blk, rows, TILE), jnp.bfloat16),
            *[
                pltpu.VMEM((panels * NEED, rows, TILE), jnp.bfloat16)
                for _ in range(ITERS * halves)
            ],
        ],
        compiler_params=pltpu.CompilerParams(
            collective_id=0, has_side_effects=True, vmem_limit_bytes=53 * 2**20
        ),
    )(tile_count, *[
        pltpu.with_memory_space_constraint(one, pltpu.HBM)
        for one in (
            tile_cols.reshape(1, slots), tile_rows.reshape(1, slots),
            decay.reshape(1, seed_count), seeds, tiles,
        )
    ])


def solution(mesh):
    in_specs = (
        P(("graph", "row"), None, None),
        P(("graph", "row")),
        P(("graph", "row")),
        P(("graph", "row")),
        P(None, ("graph", "row")),
        P(),
    )
    out_specs = P(None, ("graph", "row"))
    return jax.shard_map(
        per_device, mesh=mesh, in_specs=in_specs, out_specs=out_specs, check_vma=False
    )
```

```python
import functools

import jax
import jax.numpy as jnp
from jax import lax
from jax.experimental import pallas as pl
from jax.experimental.pallas import tpu as pltpu
from jax.sharding import PartitionSpec as P

TILE = 256
NEED = 4
HALVES = 2
PARTS = 2
ITERS = 3
MESH = pl.DeviceIdType.MESH
LANES = 128
ROW_PERM, ROW_PLACE, ROW_KEEP, ROW_LAST, ROW_HAS, ROW_COL = 0, 1, 2, 3, 4, 5


def spread(ref, slots, square):
    wide = jnp.concatenate(
        [ref[...], jnp.zeros((1, square - slots), jnp.int32)], axis=1
    ) if square > slots else ref[...]
    return jnp.broadcast_to(wide, (square, square))


def fill_wanted(cols_ref, count, wanted, slots, blk):
    width = wanted.shape[1]
    square = max(LANES, slots)
    lane = lax.broadcasted_iota(jnp.int32, (square, square), 1)
    col_row = jnp.where((lane < count) & (lane < slots), spread(cols_ref, slots, square), -1)
    col_t = jnp.transpose(col_row)[:slots, :1]
    lane_c = lax.broadcasted_iota(jnp.int32, (slots, width), 1)
    hit = (col_t == lane_c).astype(jnp.int32)
    lane_w = lax.broadcasted_iota(jnp.int32, (8, width), 1)
    local = lane_w % blk
    present = jnp.broadcast_to(jnp.max(hit, axis=0, keepdims=True), (8, width))

    def scan(value):
        step = 1
        while step < blk:
            value = value + jnp.where(local >= step, pltpu.roll(value, step, 1), 0)
            step *= 2
        return value

    rank = scan(present) - 1
    which = lax.broadcasted_iota(jnp.int32, (8, width), 0)
    chosen = (present > 0) & (rank == which)
    wanted[...] = scan(jnp.where(chosen, local, 0))
    weight = (lane_w // blk) * NEED + rank
    return hit, weight, col_t


def fill_own(rows_ref, count, own_table, hit, weight, col_t, slots, blk):
    width = hit.shape[1]
    square = max(LANES, slots)
    lane = lax.broadcasted_iota(jnp.int32, (square, square), 1)
    sub = lax.broadcasted_iota(jnp.int32, (square, square), 0)
    key_row = jnp.where(lane < count, spread(rows_ref, slots, square), blk)
    key_row = jnp.where(lane < slots, key_row, blk + 1)
    key_c = jnp.transpose(key_row)[:slots, :]
    key_r = key_row[:slots, :]
    place_col = jnp.sum(hit * weight[:1, :], axis=1, keepdims=True)
    place_col = jnp.clip(place_col, 0, (width // blk) * NEED - 1)
    lane_s, sub_s = lane[:slots, :], sub[:slots, :]
    before = (key_r < key_c) | ((key_r == key_c) & (lane_s < sub_s))
    position = jnp.sum((before & (lane_s < slots)).astype(jnp.int32), axis=1, keepdims=True)
    at = position == lane_s
    perm = jnp.sum(jnp.where(at, sub_s, 0), axis=0, keepdims=True)
    place = jnp.sum(jnp.where(at, place_col, 0), axis=0, keepdims=True)
    column = jnp.sum(jnp.where(at, jnp.clip(col_t, 0, width - 1), 0), axis=0, keepdims=True)
    key_sorted = jnp.sum(jnp.where(at, key_c, 0), axis=0, keepdims=True)
    previous = jnp.sum(jnp.where(position + 1 == lane_s, key_c, 0), axis=0, keepdims=True)
    keep = ((key_sorted == previous) & (lane_s[:1, :] > 0)).astype(jnp.int32)
    last = jnp.sum((key_c <= lane_s).astype(jnp.int32), axis=0, keepdims=True) - 1
    has = jnp.max((key_c == lane_s).astype(jnp.int32), axis=0, keepdims=True)
    own_table[...] = jnp.zeros(own_table.shape, jnp.int32)
    own_table[ROW_PERM:ROW_PERM + 1, :] = perm
    own_table[ROW_PLACE:ROW_PLACE + 1, :] = place
    own_table[ROW_KEEP:ROW_KEEP + 1, :] = keep
    own_table[ROW_LAST:ROW_LAST + 1, :] = jnp.maximum(last, 0)
    own_table[ROW_HAS:ROW_HAS + 1, :] = has
    own_table[ROW_COL:ROW_COL + 1, :] = column


def kernel(
    panels, slots, blk, seed_count, chunks, unroll, halves,
    count_ref, cols_hbm, rows_hbm, decay_hbm, seeds_hbm, tiles_hbm,
    out_ref,
    tiles, turned, seeds_ref, current, outgoing, partial, own_table, wanted, squares,
    rows_ref, cols_ref, decay_ref, own_s, wanted_s,
    whole, *arrivals,
):
    dma = pltpu.SemaphoreType.DMA
    peers, far = panels - 1, max(panels // (2 if panels % 2 == 0 else 1) - 1, 1)
    pl.run_scoped(
        functools.partial(
            body, panels, slots, blk, seed_count, chunks, unroll, halves,
            count_ref, cols_hbm, rows_hbm, decay_hbm, seeds_hbm, tiles_hbm,
            out_ref,
            tiles, turned, seeds_ref, current, outgoing, partial, own_table, wanted, squares,
            rows_ref, cols_ref, decay_ref, own_s, wanted_s, whole, arrivals,
        ),
        dma((chunks,)), dma((halves,)), dma((3,)), dma((2,)), dma((peers,)), dma((panels,)),
        dma((ITERS, halves, peers)), dma((ITERS, halves, panels)), dma((peers,)), dma((panels,)),
        dma((far, PARTS)), dma((far, PARTS)), dma((far, PARTS)), dma((far, PARTS)), dma((1,)), dma((1,)),
    )


def body(
    panels, slots, blk, seed_count, chunks, unroll, halves,
    count_ref, cols_hbm, rows_hbm, decay_hbm, seeds_hbm, tiles_hbm,
    out_ref,
    tiles, turned, seeds_ref, current, outgoing, partial, own_table, wanted, squares,
    rows_ref, cols_ref, decay_ref, own_s, wanted_s, whole, arrivals,
    tile_sem, seed_sem, small_sem, table_sem,
    want_send, want_recv, send_sem, recv_sem, norm_send, norm_recv,
    bulk_send, bulk_recv, pass_send, pass_recv, near_send, near_recv,
):
    me = lax.axis_index("row")
    cores = 2 if panels % 2 == 0 else 1
    chip, core = me // cores, me % cores
    groups = panels // cores
    rows = seed_count // halves
    peers = [
        lax.rem(chip + d, groups) * cores + e
        for d in range(groups - 1, 0, -1) for e in range(cores)
    ] + [chip * cores + lax.rem(core + e, cores) for e in range(1, cores)]

    small = [
        pltpu.make_async_copy(src, dst, small_sem.at[n])
        for n, (src, dst) in enumerate([
            (cols_hbm, cols_ref), (rows_hbm, rows_ref), (decay_hbm, decay_ref),
        ])
    ]
    for copy in small:
        copy.start()
    barrier = pltpu.get_barrier_semaphore()
    for peer in peers:
        pl.semaphore_signal(barrier, inc=1, device_id={"row": peer}, device_id_type=MESH)

    def seed_load(h):
        mine = pl.ds(h * rows, rows)
        return pltpu.make_async_copy(seeds_hbm.at[mine], seeds_ref.at[mine], seed_sem.at[h])

    for h in range(halves):
        seed_load(h).start()
    per = slots // chunks

    def load(c):
        return pltpu.make_async_copy(
            tiles_hbm.at[pl.ds(c * per, per)], tiles.at[pl.ds(c * per, per)], tile_sem.at[c]
        )

    for c in range(chunks):
        load(c).start(priority=1)

    small[0].wait()
    count = count_ref[0]
    hit, weight, col_t = fill_wanted(cols_ref, count, wanted, slots, blk)
    seed_load(0).wait()
    for b in range(blk):
        nodes = slice(b * TILE, (b + 1) * TILE)
        whole[me * blk + b] = seeds_ref[:rows, nodes].astype(jnp.bfloat16)
    pl.semaphore_wait(barrier, panels - 1)

    def ask(n, peer, source):
        return pltpu.make_async_remote_copy(
            src_ref=wanted, dst_ref=wanted_s.at[source],
            send_sem=want_send.at[n], recv_sem=want_recv.at[source],
            device_id={"row": peer}, device_id_type=MESH,
        )

    for n, peer in enumerate(peers):
        ask(n, peer, me).start()
    span = blk // PARTS
    partner = chip * cores + (cores - 1 - core)

    def block(source, part):
        return whole.at[pl.ds(source * blk + part * span, span)]

    def bulk(d, part, source):
        far = lax.rem(chip + d, groups) * cores + (cores - 1 - core)
        return pltpu.make_async_remote_copy(
            src_ref=block(source, part), dst_ref=block(source, part),
            send_sem=bulk_send.at[d - 1, part], recv_sem=bulk_recv.at[d - 1, part],
            device_id={"row": far}, device_id_type=MESH,
        )

    def hand(d, part, source):
        return pltpu.make_async_remote_copy(
            src_ref=block(source, part), dst_ref=block(source, part),
            send_sem=pass_send.at[d - 1, part], recv_sem=pass_recv.at[d - 1, part],
            device_id={"row": partner}, device_id_type=MESH,
        )

    def near(source):
        return pltpu.make_async_remote_copy(
            src_ref=whole.at[pl.ds(source * blk, blk)], dst_ref=whole.at[pl.ds(source * blk, blk)],
            send_sem=near_send.at[0], recv_sem=near_recv.at[0],
            device_id={"row": partner}, device_id_type=MESH,
        )

    def origin(d, index):
        return lax.rem(chip + groups - d, groups) * cores + index

    for part in range(PARTS):
        for d in range(1, groups):
            bulk(d, part, me).start()
    if cores > 1:
        near(me).start()
    want_copy = pltpu.make_async_copy(wanted, wanted_s.at[me], table_sem.at[1])
    want_copy.start()
    small[1].wait()
    fill_own(rows_ref, count, own_table, hit, weight, col_t, slots, blk)
    own_copy = pltpu.make_async_copy(own_table, own_s, table_sem.at[0])
    own_copy.start()
    small[2].wait()
    for h in range(1, halves):
        seed_load(h).wait()
        for b in range(blk):
            current[h, b] = seeds_ref[
                h * rows:(h + 1) * rows, b * TILE:(b + 1) * TILE
            ].astype(jnp.bfloat16)
    diagonal = lax.broadcasted_iota(jnp.int32, (seed_count, seed_count), 0) == (
        lax.broadcasted_iota(jnp.int32, (seed_count, seed_count), 1)
    )
    decay = jnp.sum(
        jnp.where(diagonal, jnp.broadcast_to(decay_ref[...], diagonal.shape), 0.0),
        axis=1, keepdims=True,
    )

    def turn(c, carry):
        load(c).wait()
        for i in range(per):
            turned[c * per + i] = jnp.transpose(tiles[c * per + i])
        return carry

    early = chunks * 8 // 8
    lax.fori_loop(0, early, turn, 0)
    for n, peer in enumerate(peers):
        ask(n, peer, peer).wait_recv()
    want_copy.wait()

    def ship(it, h, n, peer, source):
        return pltpu.make_async_remote_copy(
            src_ref=outgoing.at[it, h, n],
            dst_ref=arrivals[it * halves + h].at[pl.ds(source * NEED, NEED)],
            send_sem=send_sem.at[it, h, n], recv_sem=recv_sem.at[it, h, source],
            device_id={"row": peer}, device_id_type=MESH,
        )

    def exchange(it, h):
        arrived = arrivals[it * halves + h]
        for n, peer in enumerate(peers):
            for k in range(NEED):
                outgoing[it, h, n, k] = current[h, wanted_s[peer, k, me * blk + blk - 1]]
            ship(it, h, n, peer, me).start()
        for k in range(NEED):
            arrived[me * NEED + k] = current[h, wanted_s[me, k, me * blk + blk - 1]]

    for h in range(1, halves):
        exchange(0, h)
    lax.fori_loop(early, chunks, turn, 0)
    for part in range(PARTS):
        for d in range(1, groups):
            source = origin(d, cores - 1 - core)
            bulk(d, part, source).wait_recv()
            if cores > 1:
                hand(d, part, source).start()

    own_copy.wait()

    totals = []
    for it in range(ITERS):
        for h in range(halves):
            first = it == 0 and h == 0
            arrived = whole if first else arrivals[it * halves + h]
            row_at = ROW_COL if first else ROW_PLACE
            if first and cores > 1:
                near(partner).wait_recv()
                for part in range(PARTS):
                    for d in range(1, groups):
                        hand(d, part, origin(d, core)).wait_recv()
            if not first:
                for n, peer in enumerate(peers):
                    ship(it, h, n, peer, peer).wait_recv()

            def some(group, acc):
                for u in range(unroll):
                    j = group * unroll + u
                    product = jnp.dot(
                        arrived[own_s[row_at, j]], turned[own_s[ROW_PERM, j]],
                        preferred_element_type=jnp.float32,
                    )
                    acc = acc * own_s[ROW_KEEP, j].astype(jnp.float32) + product
                    partial[h, j] = acc
                return acc

            lax.fori_loop(0, slots // unroll, some, jnp.zeros((rows, TILE), jnp.float32))

            mine = slice(h * rows, (h + 1) * rows)
            total = jnp.zeros((rows, TILE), jnp.float32)
            for r in range(blk):
                summed = partial[h, own_s[ROW_LAST, r]] * own_s[ROW_HAS, r].astype(jnp.float32)
                value = decay[mine] * summed + seeds_ref[mine, r * TILE:(r + 1) * TILE]
                if it < ITERS - 1:
                    current[h, r] = value.astype(jnp.bfloat16)
                else:
                    out_ref[mine, r * TILE:(r + 1) * TILE] = value
                    total = total + value * value
            if it < ITERS - 1:
                exchange(it + 1, h)
            else:
                totals.append(jnp.sum(total, axis=1, keepdims=True))

    lane = lax.broadcasted_iota(jnp.int32, (8, LANES), 1)
    packed = jnp.zeros((8, LANES), jnp.float32)
    pieces = [t[i:i + 8] for t in totals for i in range(0, rows, 8)]
    for i, piece in enumerate(pieces):
        packed = jnp.where(lane == i, piece, packed)
    squares[me] = packed

    def share(n, peer, source):
        return pltpu.make_async_remote_copy(
            src_ref=squares.at[me], dst_ref=squares.at[source],
            send_sem=norm_send.at[n], recv_sem=norm_recv.at[source],
            device_id={"row": peer}, device_id_type=MESH,
        )

    for n, peer in enumerate(peers):
        share(n, peer, me).start()
    for n, peer in enumerate(peers):
        for it in range(ITERS):
            for h in range(halves):
                if (it, h) != (0, 0):
                    ship(it, h, n, peer, me).wait_send()
        ask(n, peer, me).wait_send()
    for part in range(PARTS):
        for d in range(1, groups):
            bulk(d, part, me).wait_send()
            if cores > 1:
                hand(d, part, origin(d, cores - 1 - core)).wait_send()
    if cores > 1:
        near(me).wait_send()
    for n, peer in enumerate(peers):
        share(n, peer, peer).wait_recv()
    every = squares[0]
    for p in range(1, panels):
        every = every + squares[p]
    scale = 1.0 / jnp.sqrt(every / (panels * blk * TILE) + 1e-06)
    for i in range(len(pieces)):
        one = jnp.sum(jnp.where(lane == i, scale, 0.0), axis=1, keepdims=True)
        out_ref[i * 8:(i + 1) * 8, :] = out_ref[i * 8:(i + 1) * 8, :] * one
    for n, peer in enumerate(peers):
        share(n, peer, me).wait_send()


def per_device(tiles, tile_rows, tile_cols, tile_count, seeds, decay):
    slots = tiles.shape[0]
    seed_count = seeds.shape[0]
    blk = seeds.shape[1] // TILE
    panels = lax.axis_size("row")
    width = -(-panels * blk // LANES) * LANES
    square = max(LANES, slots)
    chunks = 8 if slots % 8 == 0 else 1
    unroll = 64 if slots % 64 == 0 else 1
    halves = HALVES if seed_count % (16 * HALVES) == 0 else 1
    rows = seed_count // halves
    peers = panels - 1
    vmem = pl.BlockSpec(memory_space=pltpu.VMEM)
    return pl.pallas_call(
        functools.partial(kernel, panels, slots, blk, seed_count, chunks, unroll, halves),
        out_shape=jax.ShapeDtypeStruct(seeds.shape, jnp.float32),
        in_specs=[pl.BlockSpec(memory_space=pltpu.SMEM)] + [pl.BlockSpec(memory_space=pltpu.HBM)] * 5,
        out_specs=vmem,
        scratch_shapes=[
            pltpu.VMEM((slots, TILE, TILE), jnp.bfloat16),
            pltpu.VMEM((slots, TILE, TILE), jnp.bfloat16),
            pltpu.VMEM(seeds.shape, jnp.float32),
            pltpu.VMEM((halves, blk, rows, TILE), jnp.bfloat16),
            pltpu.VMEM((ITERS, halves, peers, NEED, rows, TILE), jnp.bfloat16),
            pltpu.VMEM((halves, slots, rows, TILE), jnp.float32),
            pltpu.VMEM((8, square), jnp.int32),
            pltpu.VMEM((8, width), jnp.int32),
            pltpu.VMEM((panels, 8, LANES), jnp.float32),
            pltpu.VMEM((1, slots), jnp.int32),
            pltpu.VMEM((1, slots), jnp.int32),
            pltpu.VMEM((1, seed_count), jnp.float32),
            pltpu.SMEM((8, square), jnp.int32),
            pltpu.SMEM((panels, 8, width), jnp.int32),
            pltpu.VMEM((panels * blk, rows, TILE), jnp.bfloat16),
            *[
                pltpu.VMEM((panels * NEED, rows, TILE), jnp.bfloat16)
                for _ in range(ITERS * halves)
            ],
        ],
        compiler_params=pltpu.CompilerParams(
            collective_id=0, has_side_effects=True, vmem_limit_bytes=53 * 2**20
        ),
    )(tile_count, *[
        pltpu.with_memory_space_constraint(one, pltpu.HBM)
        for one in (
            tile_cols.reshape(1, slots), tile_rows.reshape(1, slots),
            decay.reshape(1, seed_count), seeds, tiles,
        )
    ])


def solution(mesh):
    in_specs = (
        P(("graph", "row"), None, None),
        P(("graph", "row")),
        P(("graph", "row")),
        P(("graph", "row")),
        P(None, ("graph", "row")),
        P(),
    )
    out_specs = P(None, ("graph", "row"))
    return jax.shard_map(
        per_device, mesh=mesh, in_specs=in_specs, out_specs=out_specs, check_vma=False
    )
```

```python
import functools

import jax
import jax.numpy as jnp
from jax import lax
from jax.experimental import pallas as pl
from jax.experimental.pallas import tpu as pltpu
from jax.sharding import PartitionSpec as P

TILE = 256
NEED = 4
HALVES = 2
PARTS = 2
TAIL = 8
ITERS = 3
MESH = pl.DeviceIdType.MESH
LANES = 128
CUTS = TILE // LANES
ROW_PERM, ROW_PLACE, ROW_KEEP, ROW_LAST, ROW_HAS, ROW_COL = 0, 1, 2, 3, 4, 5


def spread(ref, slots, square):
    wide = jnp.concatenate(
        [ref[...], jnp.zeros((1, square - slots), jnp.int32)], axis=1
    ) if square > slots else ref[...]
    return jnp.broadcast_to(wide, (square, square))


def fill_wanted(cols_ref, count, wanted, slots, blk):
    width = wanted.shape[1]
    square = max(LANES, slots)
    lane = lax.broadcasted_iota(jnp.int32, (square, square), 1)
    col_row = jnp.where((lane < count) & (lane < slots), spread(cols_ref, slots, square), -1)
    col_t = jnp.transpose(col_row)[:slots, :1]
    lane_c = lax.broadcasted_iota(jnp.int32, (slots, width), 1)
    hit = (col_t == lane_c).astype(jnp.int32)
    lane_w = lax.broadcasted_iota(jnp.int32, (8, width), 1)
    local = lane_w % blk
    present = jnp.broadcast_to(jnp.max(hit, axis=0, keepdims=True), (8, width))

    def scan(value):
        step = 1
        while step < blk:
            value = value + jnp.where(local >= step, pltpu.roll(value, step, 1), 0)
            step *= 2
        return value

    rank = scan(present) - 1
    which = lax.broadcasted_iota(jnp.int32, (8, width), 0)
    chosen = (present > 0) & (rank == which)
    wanted[...] = scan(jnp.where(chosen, local, 0))
    weight = (lane_w // blk) * NEED + rank
    return hit, weight, col_t


def fill_own(rows_ref, count, own_table, hit, weight, col_t, slots, blk):
    width = hit.shape[1]
    square = max(LANES, slots)
    lane = lax.broadcasted_iota(jnp.int32, (square, square), 1)
    sub = lax.broadcasted_iota(jnp.int32, (square, square), 0)
    key_row = jnp.where(lane < count, spread(rows_ref, slots, square), blk)
    key_row = jnp.where(lane < slots, key_row, blk + 1)
    key_c = jnp.transpose(key_row)[:slots, :]
    key_r = key_row[:slots, :]
    place_col = jnp.sum(hit * weight[:1, :], axis=1, keepdims=True)
    place_col = jnp.clip(place_col, 0, (width // blk) * NEED - 1)
    lane_s, sub_s = lane[:slots, :], sub[:slots, :]
    before = (key_r < key_c) | ((key_r == key_c) & (lane_s < sub_s))
    position = jnp.sum((before & (lane_s < slots)).astype(jnp.int32), axis=1, keepdims=True)
    at = position == lane_s
    perm = jnp.sum(jnp.where(at, sub_s, 0), axis=0, keepdims=True)
    place = jnp.sum(jnp.where(at, place_col, 0), axis=0, keepdims=True)
    column = jnp.sum(jnp.where(at, jnp.clip(col_t, 0, width - 1), 0), axis=0, keepdims=True)
    key_sorted = jnp.sum(jnp.where(at, key_c, 0), axis=0, keepdims=True)
    previous = jnp.sum(jnp.where(position + 1 == lane_s, key_c, 0), axis=0, keepdims=True)
    keep = ((key_sorted == previous) & (lane_s[:1, :] > 0)).astype(jnp.int32)
    last = jnp.sum((key_c <= lane_s).astype(jnp.int32), axis=0, keepdims=True) - 1
    has = jnp.max((key_c == lane_s).astype(jnp.int32), axis=0, keepdims=True)
    own_table[...] = jnp.zeros(own_table.shape, jnp.int32)
    own_table[ROW_PERM:ROW_PERM + 1, :] = perm
    own_table[ROW_PLACE:ROW_PLACE + 1, :] = place
    own_table[ROW_KEEP:ROW_KEEP + 1, :] = keep
    own_table[ROW_LAST:ROW_LAST + 1, :] = jnp.maximum(last, 0)
    own_table[ROW_HAS:ROW_HAS + 1, :] = has
    own_table[ROW_COL:ROW_COL + 1, :] = column


def kernel(
    panels, slots, blk, seed_count, chunks, halves,
    count_ref, cols_hbm, rows_hbm, decay_hbm, seeds_hbm, tiles_hbm,
    out_ref,
    tiles, turned, seeds_ref, current, outgoing, partial, own_table, wanted, squares,
    rows_ref, cols_ref, decay_ref, own_s, wanted_s,
    whole, *arrivals,
):
    dma = pltpu.SemaphoreType.DMA
    peers, far = panels - 1, max(panels // (2 if panels % 2 == 0 else 1) - 1, 1)
    pl.run_scoped(
        functools.partial(
            body, panels, slots, blk, seed_count, chunks, halves,
            count_ref, cols_hbm, rows_hbm, decay_hbm, seeds_hbm, tiles_hbm,
            out_ref,
            tiles, turned, seeds_ref, current, outgoing, partial, own_table, wanted, squares,
            rows_ref, cols_ref, decay_ref, own_s, wanted_s, whole, arrivals,
        ),
        dma((chunks,)), dma((halves,)), dma((3,)), dma((2,)), dma((peers,)), dma((panels,)),
        dma((ITERS, halves, CUTS, peers)), dma((ITERS, halves, CUTS, panels)), dma((peers,)), dma((panels,)),
        dma((far, PARTS)), dma((far, PARTS)), dma((far, PARTS)), dma((far, PARTS)), dma((1,)), dma((1,)),
    )


def body(
    panels, slots, blk, seed_count, chunks, halves,
    count_ref, cols_hbm, rows_hbm, decay_hbm, seeds_hbm, tiles_hbm,
    out_ref,
    tiles, turned, seeds_ref, current, outgoing, partial, own_table, wanted, squares,
    rows_ref, cols_ref, decay_ref, own_s, wanted_s, whole, arrivals,
    tile_sem, seed_sem, small_sem, table_sem,
    want_send, want_recv, send_sem, recv_sem, norm_send, norm_recv,
    bulk_send, bulk_recv, pass_send, pass_recv, near_send, near_recv,
):
    me = lax.axis_index("row")
    cores = 2 if panels % 2 == 0 else 1
    chip, core = me // cores, me % cores
    groups = panels // cores
    rows = seed_count // halves
    peers = [
        lax.rem(chip + d, groups) * cores + e
        for d in range(groups - 1, 0, -1) for e in range(cores)
    ] + [chip * cores + lax.rem(core + e, cores) for e in range(1, cores)]
    away = (groups - 1) * cores

    small = [
        pltpu.make_async_copy(src, dst, small_sem.at[n])
        for n, (src, dst) in enumerate([
            (cols_hbm, cols_ref), (rows_hbm, rows_ref), (decay_hbm, decay_ref),
        ])
    ]
    for copy in small:
        copy.start()
    barrier = pltpu.get_barrier_semaphore()
    for peer in peers:
        pl.semaphore_signal(barrier, inc=1, device_id={"row": peer}, device_id_type=MESH)

    def seed_load(h):
        mine = pl.ds(h * rows, rows)
        return pltpu.make_async_copy(seeds_hbm.at[mine], seeds_ref.at[mine], seed_sem.at[h])

    for h in range(halves):
        seed_load(h).start()
    per = slots // chunks

    def load(c):
        return pltpu.make_async_copy(
            tiles_hbm.at[pl.ds(c * per, per)], tiles.at[pl.ds(c * per, per)], tile_sem.at[c]
        )

    for c in range(chunks):
        load(c).start(priority=1)

    small[0].wait()
    count = count_ref[0]
    hit, weight, col_t = fill_wanted(cols_ref, count, wanted, slots, blk)
    seed_load(0).wait()
    for b in range(blk):
        nodes = slice(b * TILE, (b + 1) * TILE)
        whole[me * blk + b] = seeds_ref[:rows, nodes].astype(jnp.bfloat16)
    pl.semaphore_wait(barrier, panels - 1)

    def ask(n, peer, source):
        return pltpu.make_async_remote_copy(
            src_ref=wanted, dst_ref=wanted_s.at[source],
            send_sem=want_send.at[n], recv_sem=want_recv.at[source],
            device_id={"row": peer}, device_id_type=MESH,
        )

    for n, peer in enumerate(peers):
        ask(n, peer, me).start()
    span = blk // PARTS
    partner = chip * cores + (cores - 1 - core)

    def block(source, part):
        return whole.at[pl.ds(source * blk + part * span, span)]

    def bulk(d, part, source):
        far = lax.rem(chip + d, groups) * cores + (cores - 1 - core)
        return pltpu.make_async_remote_copy(
            src_ref=block(source, part), dst_ref=block(source, part),
            send_sem=bulk_send.at[d - 1, part], recv_sem=bulk_recv.at[d - 1, part],
            device_id={"row": far}, device_id_type=MESH,
        )

    def hand(d, part, source):
        return pltpu.make_async_remote_copy(
            src_ref=block(source, part), dst_ref=block(source, part),
            send_sem=pass_send.at[d - 1, part], recv_sem=pass_recv.at[d - 1, part],
            device_id={"row": partner}, device_id_type=MESH,
        )

    def near(source):
        return pltpu.make_async_remote_copy(
            src_ref=whole.at[pl.ds(source * blk, blk)], dst_ref=whole.at[pl.ds(source * blk, blk)],
            send_sem=near_send.at[0], recv_sem=near_recv.at[0],
            device_id={"row": partner}, device_id_type=MESH,
        )

    def origin(d, index):
        return lax.rem(chip + groups - d, groups) * cores + index

    for part in range(PARTS):
        for d in range(1, groups):
            bulk(d, part, me).start()
    if cores > 1:
        near(me).start()
    want_copy = pltpu.make_async_copy(wanted, wanted_s.at[me], table_sem.at[1])
    want_copy.start()
    small[1].wait()
    fill_own(rows_ref, count, own_table, hit, weight, col_t, slots, blk)
    own_copy = pltpu.make_async_copy(own_table, own_s, table_sem.at[0])
    own_copy.start()
    small[2].wait()
    for h in range(1, halves):
        seed_load(h).wait()
        for b in range(blk):
            for k in range(CUTS):
                current[h, k, b] = seeds_ref[
                    h * rows:(h + 1) * rows, b * TILE + k * LANES:b * TILE + (k + 1) * LANES
                ].astype(jnp.bfloat16)
    diagonal = lax.broadcasted_iota(jnp.int32, (seed_count, seed_count), 0) == (
        lax.broadcasted_iota(jnp.int32, (seed_count, seed_count), 1)
    )
    decay = jnp.sum(
        jnp.where(diagonal, jnp.broadcast_to(decay_ref[...], diagonal.shape), 0.0),
        axis=1, keepdims=True,
    )

    def turn(c, carry):
        load(c).wait()
        for i in range(per):
            turned[c * per + i] = jnp.transpose(tiles[c * per + i])
        return carry

    early = chunks * 8 // 8
    lax.fori_loop(0, early, turn, 0)
    for n, peer in enumerate(peers):
        ask(n, peer, peer).wait_recv()
    want_copy.wait()

    def ship(it, h, k, n, peer, source):
        return pltpu.make_async_remote_copy(
            src_ref=outgoing.at[it, h, k, n],
            dst_ref=arrivals[(it * halves + h) * CUTS + k].at[pl.ds(source * NEED, NEED)],
            send_sem=send_sem.at[it, h, k, n], recv_sem=recv_sem.at[it, h, k, source],
            device_id={"row": peer}, device_id_type=MESH,
        )

    def exchange(it, h, k):
        arrived = arrivals[(it * halves + h) * CUTS + k]
        last = k == CUTS - 1
        for n, peer in enumerate(peers[:away]):
            for w in range(NEED):
                outgoing[it, h, k, n, w] = current[h, k, wanted_s[peer, w, me * blk + blk - 1]]
            ship(it, h, k, n, peer, me).start()
        for c in range(CUTS) if last else ():
            for n, peer in list(enumerate(peers))[away:]:
                for w in range(NEED):
                    outgoing[it, h, c, n, w] = current[h, c, wanted_s[peer, w, me * blk + blk - 1]]
                ship(it, h, c, n, peer, me).start()
        for w in range(NEED):
            arrived[me * NEED + w] = current[h, k, wanted_s[me, w, me * blk + blk - 1]]

    for h in range(1, halves):
        for k in range(CUTS):
            exchange(0, h, k)
    lax.fori_loop(early, chunks, turn, 0)
    for part in range(PARTS):
        for d in range(1, groups):
            source = origin(d, cores - 1 - core)
            bulk(d, part, source).wait_recv()
            if cores > 1:
                hand(d, part, source).start()

    own_copy.wait()

    totals = []
    for it in range(ITERS):
        for h in range(halves):
            first = it == 0 and h == 0
            def contract(arrived, place, k, nodes, some, acc):
                for j in some:
                    product = jnp.dot(
                        arrived[own_s[place, j]],
                        turned[own_s[ROW_PERM, j], nodes, :],
                        preferred_element_type=jnp.float32,
                    )
                    acc = acc * own_s[ROW_KEEP, j].astype(jnp.float32) + product
                    partial[h, k, j] = acc
                return acc

            zero = jnp.zeros((rows, TILE), jnp.float32)
            if first:
                if cores > 1:
                    near(partner).wait_recv()
                    for part in range(PARTS):
                        for d in range(1, groups):
                            hand(d, part, origin(d, core)).wait_recv()
                contract(whole, ROW_COL, 0, slice(0, TILE), range(slots), zero)
            else:
                rest = range(0)
                for k in range(CUTS):
                    for n, peer in enumerate(peers):
                        ship(it, h, k, n, peer, peer).wait_recv()
                    if k > 0:
                        contract(*use, rest, acc)
                    use = (
                        arrivals[(it * halves + h) * CUTS + k], ROW_PLACE, k,
                        slice(k * LANES, (k + 1) * LANES),
                    )
                    cut = slots - TAIL if k < CUTS - 1 else slots
                    acc = contract(*use, range(cut), zero)
                    rest = range(cut, slots)

            mine = slice(h * rows, (h + 1) * rows)
            total = jnp.zeros((rows, LANES), jnp.float32)
            for k in range(CUTS):
                out = slice(k * LANES, (k + 1) * LANES)
                for r in range(blk):
                    last = own_s[ROW_LAST, r]
                    summed = partial[h, 0, last, :, out]
                    for c in range(1, 1 if first else CUTS):
                        summed = summed + partial[h, c, last, :, out]
                    summed = summed * own_s[ROW_HAS, r].astype(jnp.float32)
                    nodes = slice(r * TILE + k * LANES, r * TILE + (k + 1) * LANES)
                    value = decay[mine] * summed + seeds_ref[mine, nodes]
                    if it < ITERS - 1:
                        current[h, k, r] = value.astype(jnp.bfloat16)
                    else:
                        out_ref[mine, nodes] = value
                        total = total + value * value
                if it < ITERS - 1:
                    exchange(it + 1, h, k)
            if it == ITERS - 1:
                totals.append(jnp.sum(total, axis=1, keepdims=True))

    lane = lax.broadcasted_iota(jnp.int32, (8, LANES), 1)
    packed = jnp.zeros((8, LANES), jnp.float32)
    pieces = [t[i:i + 8] for t in totals for i in range(0, rows, 8)]
    for i, piece in enumerate(pieces):
        packed = jnp.where(lane == i, piece, packed)
    squares[me] = packed

    def share(n, peer, source):
        return pltpu.make_async_remote_copy(
            src_ref=squares.at[me], dst_ref=squares.at[source],
            send_sem=norm_send.at[n], recv_sem=norm_recv.at[source],
            device_id={"row": peer}, device_id_type=MESH,
        )

    for n, peer in enumerate(peers):
        share(n, peer, me).start()
    for n, peer in enumerate(peers):
        for it in range(ITERS):
            for h in range(halves):
                for k in range(CUTS):
                    if (it, h) != (0, 0):
                        ship(it, h, k, n, peer, me).wait_send()
        ask(n, peer, me).wait_send()
    for part in range(PARTS):
        for d in range(1, groups):
            bulk(d, part, me).wait_send()
            if cores > 1:
                hand(d, part, origin(d, cores - 1 - core)).wait_send()
    if cores > 1:
        near(me).wait_send()
    for n, peer in enumerate(peers):
        share(n, peer, peer).wait_recv()
    every = squares[0]
    for p in range(1, panels):
        every = every + squares[p]
    scale = 1.0 / jnp.sqrt(every / (panels * blk * TILE) + 1e-06)
    for i in range(len(pieces)):
        one = jnp.sum(jnp.where(lane == i, scale, 0.0), axis=1, keepdims=True)
        out_ref[i * 8:(i + 1) * 8, :] = out_ref[i * 8:(i + 1) * 8, :] * one
    for n, peer in enumerate(peers):
        share(n, peer, me).wait_send()


def per_device(tiles, tile_rows, tile_cols, tile_count, seeds, decay):
    slots = tiles.shape[0]
    seed_count = seeds.shape[0]
    blk = seeds.shape[1] // TILE
    panels = lax.axis_size("row")
    width = -(-panels * blk // LANES) * LANES
    square = max(LANES, slots)
    chunks = 8 if slots % 8 == 0 else 1
    halves = HALVES if seed_count % (16 * HALVES) == 0 else 1
    rows = seed_count // halves
    peers = panels - 1
    vmem = pl.BlockSpec(memory_space=pltpu.VMEM)
    return pl.pallas_call(
        functools.partial(kernel, panels, slots, blk, seed_count, chunks, halves),
        out_shape=jax.ShapeDtypeStruct(seeds.shape, jnp.float32),
        in_specs=[pl.BlockSpec(memory_space=pltpu.SMEM)] + [pl.BlockSpec(memory_space=pltpu.HBM)] * 5,
        out_specs=vmem,
        scratch_shapes=[
            pltpu.VMEM((slots, TILE, TILE), jnp.bfloat16),
            pltpu.VMEM((slots, TILE, TILE), jnp.bfloat16),
            pltpu.VMEM(seeds.shape, jnp.float32),
            pltpu.VMEM((halves, CUTS, blk, rows, LANES), jnp.bfloat16),
            pltpu.VMEM((ITERS, halves, CUTS, peers, NEED, rows, LANES), jnp.bfloat16),
            pltpu.VMEM((halves, CUTS, slots, rows, TILE), jnp.float32),
            pltpu.VMEM((8, square), jnp.int32),
            pltpu.VMEM((8, width), jnp.int32),
            pltpu.VMEM((panels, 8, LANES), jnp.float32),
            pltpu.VMEM((1, slots), jnp.int32),
            pltpu.VMEM((1, slots), jnp.int32),
            pltpu.VMEM((1, seed_count), jnp.float32),
            pltpu.SMEM((8, square), jnp.int32),
            pltpu.SMEM((panels, 8, width), jnp.int32),
            pltpu.VMEM((panels * blk, rows, TILE), jnp.bfloat16),
            *[
                pltpu.VMEM((panels * NEED, rows, LANES), jnp.bfloat16)
                for _ in range(ITERS * halves * CUTS)
            ],
        ],
        compiler_params=pltpu.CompilerParams(
            collective_id=0, has_side_effects=True, vmem_limit_bytes=53 * 2**20
        ),
    )(tile_count, *[
        pltpu.with_memory_space_constraint(one, pltpu.HBM)
        for one in (
            tile_cols.reshape(1, slots), tile_rows.reshape(1, slots),
            decay.reshape(1, seed_count), seeds, tiles,
        )
    ])


def solution(mesh):
    in_specs = (
        P(("graph", "row"), None, None),
        P(("graph", "row")),
        P(("graph", "row")),
        P(("graph", "row")),
        P(None, ("graph", "row")),
        P(),
    )
    out_specs = P(None, ("graph", "row"))
    return jax.shard_map(
        per_device, mesh=mesh, in_specs=in_specs, out_specs=out_specs, check_vma=False
    )
```

```python
import functools

import jax
import jax.numpy as jnp
from jax import lax
from jax.experimental import pallas as pl
from jax.experimental.pallas import tpu as pltpu
from jax.sharding import PartitionSpec as P

TILE = 256
NEED = 4
HALVES = 2
TAIL = 8
ITERS = 3
MESH = pl.DeviceIdType.MESH
LANES = 128
CUTS = TILE // LANES
ROW_PERM, ROW_PLACE, ROW_KEEP, ROW_LAST, ROW_HAS, ROW_COL = 0, 1, 2, 3, 4, 5


def spread(ref, slots, square):
    wide = jnp.concatenate(
        [ref[...], jnp.zeros((1, square - slots), jnp.int32)], axis=1
    ) if square > slots else ref[...]
    return jnp.broadcast_to(wide, (square, square))


def fill_wanted(cols_ref, count, wanted, slots, blk):
    width = wanted.shape[1]
    square = max(LANES, slots)
    lane = lax.broadcasted_iota(jnp.int32, (square, square), 1)
    col_row = jnp.where((lane < count) & (lane < slots), spread(cols_ref, slots, square), -1)
    col_t = jnp.transpose(col_row)[:slots, :1]
    lane_c = lax.broadcasted_iota(jnp.int32, (slots, width), 1)
    hit = (col_t == lane_c).astype(jnp.int32)
    lane_w = lax.broadcasted_iota(jnp.int32, (8, width), 1)
    local = lane_w % blk
    present = jnp.broadcast_to(jnp.max(hit, axis=0, keepdims=True), (8, width))

    def scan(value):
        step = 1
        while step < blk:
            value = value + jnp.where(local >= step, pltpu.roll(value, step, 1), 0)
            step *= 2
        return value

    rank = scan(present) - 1
    which = lax.broadcasted_iota(jnp.int32, (8, width), 0)
    chosen = (present > 0) & (rank == which)
    wanted[...] = scan(jnp.where(chosen, local, 0))
    weight = (lane_w // blk) * NEED + rank
    return hit, weight, col_t


def fill_own(rows_ref, count, own_table, hit, weight, col_t, slots, blk):
    width = hit.shape[1]
    square = max(LANES, slots)
    lane = lax.broadcasted_iota(jnp.int32, (square, square), 1)
    sub = lax.broadcasted_iota(jnp.int32, (square, square), 0)
    key_row = jnp.where(lane < count, spread(rows_ref, slots, square), blk)
    key_row = jnp.where(lane < slots, key_row, blk + 1)
    key_c = jnp.transpose(key_row)[:slots, :]
    key_r = key_row[:slots, :]
    place_col = jnp.sum(hit * weight[:1, :], axis=1, keepdims=True)
    place_col = jnp.clip(place_col, 0, (width // blk) * NEED - 1)
    lane_s, sub_s = lane[:slots, :], sub[:slots, :]
    before = (key_r < key_c) | ((key_r == key_c) & (lane_s < sub_s))
    position = jnp.sum((before & (lane_s < slots)).astype(jnp.int32), axis=1, keepdims=True)
    at = position == lane_s
    perm = jnp.sum(jnp.where(at, sub_s, 0), axis=0, keepdims=True)
    place = jnp.sum(jnp.where(at, place_col, 0), axis=0, keepdims=True)
    column = jnp.sum(jnp.where(at, jnp.clip(col_t, 0, width - 1), 0), axis=0, keepdims=True)
    key_sorted = jnp.sum(jnp.where(at, key_c, 0), axis=0, keepdims=True)
    previous = jnp.sum(jnp.where(position + 1 == lane_s, key_c, 0), axis=0, keepdims=True)
    keep = ((key_sorted == previous) & (lane_s[:1, :] > 0)).astype(jnp.int32)
    last = jnp.sum((key_c <= lane_s).astype(jnp.int32), axis=0, keepdims=True) - 1
    has = jnp.max((key_c == lane_s).astype(jnp.int32), axis=0, keepdims=True)
    own_table[...] = jnp.zeros(own_table.shape, jnp.int32)
    own_table[ROW_PERM:ROW_PERM + 1, :] = perm
    own_table[ROW_PLACE:ROW_PLACE + 1, :] = place
    own_table[ROW_KEEP:ROW_KEEP + 1, :] = keep
    own_table[ROW_LAST:ROW_LAST + 1, :] = jnp.maximum(last, 0)
    own_table[ROW_HAS:ROW_HAS + 1, :] = has
    own_table[ROW_COL:ROW_COL + 1, :] = column


def kernel(
    panels, slots, blk, seed_count, chunks, halves,
    count_ref, cols_hbm, rows_hbm, decay_hbm, seeds_hbm, tiles_hbm,
    out_ref,
    tiles, turned, seeds_ref, current, outgoing, partial, own_table, wanted, squares,
    rows_ref, cols_ref, decay_ref, own_s, wanted_s,
    *landing,
):
    whole, arrivals = landing[:CUTS], landing[CUTS:]
    dma = pltpu.SemaphoreType.DMA
    peers, far = panels - 1, max(panels // (2 if panels % 2 == 0 else 1) - 1, 1)
    pl.run_scoped(
        functools.partial(
            body, panels, slots, blk, seed_count, chunks, halves,
            count_ref, cols_hbm, rows_hbm, decay_hbm, seeds_hbm, tiles_hbm,
            out_ref,
            tiles, turned, seeds_ref, current, outgoing, partial, own_table, wanted, squares,
            rows_ref, cols_ref, decay_ref, own_s, wanted_s, whole, arrivals,
        ),
        dma((chunks,)), dma((halves,)), dma((3,)), dma((2,)), dma((peers,)), dma((panels,)),
        dma((ITERS, halves, CUTS, peers)), dma((ITERS, halves, CUTS, panels)), dma((peers,)), dma((panels,)),
        dma((far, CUTS)), dma((far, CUTS)), dma((far, CUTS)), dma((far, CUTS)), dma((CUTS,)), dma((CUTS,)),
    )


def body(
    panels, slots, blk, seed_count, chunks, halves,
    count_ref, cols_hbm, rows_hbm, decay_hbm, seeds_hbm, tiles_hbm,
    out_ref,
    tiles, turned, seeds_ref, current, outgoing, partial, own_table, wanted, squares,
    rows_ref, cols_ref, decay_ref, own_s, wanted_s, whole, arrivals,
    tile_sem, seed_sem, small_sem, table_sem,
    want_send, want_recv, send_sem, recv_sem, norm_send, norm_recv,
    bulk_send, bulk_recv, pass_send, pass_recv, near_send, near_recv,
):
    me = lax.axis_index("row")
    cores = 2 if panels % 2 == 0 else 1
    chip, core = me // cores, me % cores
    groups = panels // cores
    rows = seed_count // halves
    peers = [
        lax.rem(chip + d, groups) * cores + e
        for d in range(groups - 1, 0, -1) for e in range(cores)
    ] + [chip * cores + lax.rem(core + e, cores) for e in range(1, cores)]
    away = (groups - 1) * cores

    small = [
        pltpu.make_async_copy(src, dst, small_sem.at[n])
        for n, (src, dst) in enumerate([
            (cols_hbm, cols_ref), (rows_hbm, rows_ref), (decay_hbm, decay_ref),
        ])
    ]
    for copy in small:
        copy.start()
    barrier = pltpu.get_barrier_semaphore()
    for peer in peers:
        pl.semaphore_signal(barrier, inc=1, device_id={"row": peer}, device_id_type=MESH)

    def seed_load(h):
        mine = pl.ds(h * rows, rows)
        return pltpu.make_async_copy(seeds_hbm.at[mine], seeds_ref.at[mine], seed_sem.at[h])

    for h in range(halves):
        seed_load(h).start()
    per = slots // chunks

    def load(c):
        return pltpu.make_async_copy(
            tiles_hbm.at[pl.ds(c * per, per)], tiles.at[pl.ds(c * per, per)], tile_sem.at[c]
        )

    for c in range(chunks):
        load(c).start(priority=1)

    small[0].wait()
    count = count_ref[0]
    hit, weight, col_t = fill_wanted(cols_ref, count, wanted, slots, blk)
    seed_load(0).wait()
    for b in range(blk):
        for k in range(CUTS):
            nodes = slice(b * TILE + k * LANES, b * TILE + (k + 1) * LANES)
            whole[k][me * blk + b] = seeds_ref[:rows, nodes].astype(jnp.bfloat16)
    pl.semaphore_wait(barrier, panels - 1)

    def ask(n, peer, source):
        return pltpu.make_async_remote_copy(
            src_ref=wanted.at[pl.ds(0, NEED)], dst_ref=wanted_s.at[source, pl.ds(0, NEED)],
            send_sem=want_send.at[n], recv_sem=want_recv.at[source],
            device_id={"row": peer}, device_id_type=MESH,
        )

    for n, peer in enumerate(peers):
        ask(n, peer, me).start()
    partner = chip * cores + (cores - 1 - core)

    def block(source, part):
        return whole[part].at[pl.ds(source * blk, blk)]

    def bulk(d, part, source):
        far = lax.rem(chip + d, groups) * cores + (cores - 1 - core)
        return pltpu.make_async_remote_copy(
            src_ref=block(source, part), dst_ref=block(source, part),
            send_sem=bulk_send.at[d - 1, part], recv_sem=bulk_recv.at[d - 1, part],
            device_id={"row": far}, device_id_type=MESH,
        )

    def hand(d, part, source):
        return pltpu.make_async_remote_copy(
            src_ref=block(source, part), dst_ref=block(source, part),
            send_sem=pass_send.at[d - 1, part], recv_sem=pass_recv.at[d - 1, part],
            device_id={"row": partner}, device_id_type=MESH,
        )

    def near(part, source):
        return pltpu.make_async_remote_copy(
            src_ref=block(source, part), dst_ref=block(source, part),
            send_sem=near_send.at[part], recv_sem=near_recv.at[part],
            device_id={"row": partner}, device_id_type=MESH,
        )

    def origin(d, index):
        return lax.rem(chip + groups - d, groups) * cores + index

    for part in range(CUTS):
        for d in range(1, groups):
            bulk(d, part, me).start()
    if cores > 1:
        for part in range(CUTS):
            near(part, me).start()
    want_copy = pltpu.make_async_copy(wanted, wanted_s.at[me], table_sem.at[1])
    want_copy.start()
    small[1].wait()
    fill_own(rows_ref, count, own_table, hit, weight, col_t, slots, blk)
    own_copy = pltpu.make_async_copy(own_table, own_s, table_sem.at[0])
    own_copy.start()
    small[2].wait()
    for h in range(1, halves):
        seed_load(h).wait()
        for b in range(blk):
            for k in range(CUTS):
                current[h, k, b] = seeds_ref[
                    h * rows:(h + 1) * rows, b * TILE + k * LANES:b * TILE + (k + 1) * LANES
                ].astype(jnp.bfloat16)
    diagonal = lax.broadcasted_iota(jnp.int32, (seed_count, seed_count), 0) == (
        lax.broadcasted_iota(jnp.int32, (seed_count, seed_count), 1)
    )
    decay = jnp.sum(
        jnp.where(diagonal, jnp.broadcast_to(decay_ref[...], diagonal.shape), 0.0),
        axis=1, keepdims=True,
    )

    def turn(c, carry):
        load(c).wait()
        for i in range(per):
            turned[c * per + i] = jnp.transpose(tiles[c * per + i])
        return carry

    early = chunks * 8 // 8
    lax.fori_loop(0, early, turn, 0)
    for n, peer in enumerate(peers):
        ask(n, peer, peer).wait_recv()
    want_copy.wait()

    def ship(it, h, k, n, peer, source):
        return pltpu.make_async_remote_copy(
            src_ref=outgoing.at[it, h, k, n],
            dst_ref=arrivals[(it * halves + h) * CUTS + k].at[pl.ds(source * NEED, NEED)],
            send_sem=send_sem.at[it, h, k, n], recv_sem=recv_sem.at[it, h, k, source],
            device_id={"row": peer}, device_id_type=MESH,
        )

    def exchange(it, h, k):
        arrived = arrivals[(it * halves + h) * CUTS + k]
        last = k == CUTS - 1
        for n, peer in enumerate(peers[:away]):
            for w in range(NEED):
                outgoing[it, h, k, n, w] = current[h, k, wanted_s[peer, w, me * blk + blk - 1]]
            ship(it, h, k, n, peer, me).start()
        for c in range(CUTS) if last else ():
            for n, peer in list(enumerate(peers))[away:]:
                for w in range(NEED):
                    outgoing[it, h, c, n, w] = current[h, c, wanted_s[peer, w, me * blk + blk - 1]]
                ship(it, h, c, n, peer, me).start()
        for w in range(NEED):
            arrived[me * NEED + w] = current[h, k, wanted_s[me, w, me * blk + blk - 1]]

    for h in range(1, halves):
        for k in range(CUTS):
            exchange(0, h, k)
    lax.fori_loop(early, chunks, turn, 0)
    for part in range(CUTS):
        for d in range(1, groups):
            source = origin(d, cores - 1 - core)
            bulk(d, part, source).wait_recv()
            if cores > 1:
                hand(d, part, source).start()

    own_copy.wait()

    totals = []
    for it in range(ITERS):
        for h in range(halves):
            first = it == 0 and h == 0
            def contract(arrived, place, k, nodes, some, acc):
                for j in some:
                    product = jnp.dot(
                        arrived[own_s[place, j]],
                        turned[own_s[ROW_PERM, j], nodes, :],
                        preferred_element_type=jnp.float32,
                    )
                    acc = acc * own_s[ROW_KEEP, j].astype(jnp.float32) + product
                    partial[h, k, j] = acc
                return acc

            zero = jnp.zeros((rows, TILE), jnp.float32)
            def arrive(k):
                if not first:
                    for n, peer in enumerate(peers):
                        ship(it, h, k, n, peer, peer).wait_recv()
                elif cores > 1:
                    near(k, partner).wait_recv()
                    for d in range(1, groups):
                        hand(d, k, origin(d, core)).wait_recv()

            rest = range(0)
            for k in range(CUTS):
                arrive(k)
                if k > 0:
                    contract(*use, rest, acc)
                use = (
                    whole[k] if first else arrivals[(it * halves + h) * CUTS + k],
                    ROW_COL if first else ROW_PLACE, k, slice(k * LANES, (k + 1) * LANES),
                )
                cut = slots - TAIL if k < CUTS - 1 else slots
                acc = contract(*use, range(cut), zero)
                rest = range(cut, slots)

            mine = slice(h * rows, (h + 1) * rows)
            total = jnp.zeros((rows, LANES), jnp.float32)
            for k in range(CUTS):
                out = slice(k * LANES, (k + 1) * LANES)
                for r in range(blk):
                    last = own_s[ROW_LAST, r]
                    summed = partial[h, 0, last, :, out]
                    for c in range(1, CUTS):
                        summed = summed + partial[h, c, last, :, out]
                    summed = summed * own_s[ROW_HAS, r].astype(jnp.float32)
                    nodes = slice(r * TILE + k * LANES, r * TILE + (k + 1) * LANES)
                    value = decay[mine] * summed + seeds_ref[mine, nodes]
                    if it < ITERS - 1:
                        current[h, k, r] = value.astype(jnp.bfloat16)
                    else:
                        out_ref[mine, nodes] = value
                        total = total + value * value
                if it < ITERS - 1:
                    exchange(it + 1, h, k)
            if it == ITERS - 1:
                totals.append(jnp.sum(total, axis=1, keepdims=True))

    lane = lax.broadcasted_iota(jnp.int32, (8, LANES), 1)
    packed = jnp.zeros((8, LANES), jnp.float32)
    pieces = [t[i:i + 8] for t in totals for i in range(0, rows, 8)]
    for i, piece in enumerate(pieces):
        packed = jnp.where(lane == i, piece, packed)
    squares[me] = packed

    def share(n, peer, source):
        return pltpu.make_async_remote_copy(
            src_ref=squares.at[me], dst_ref=squares.at[source],
            send_sem=norm_send.at[n], recv_sem=norm_recv.at[source],
            device_id={"row": peer}, device_id_type=MESH,
        )

    for n, peer in enumerate(peers):
        share(n, peer, me).start()
    for n, peer in enumerate(peers):
        for it in range(ITERS):
            for h in range(halves):
                for k in range(CUTS):
                    if (it, h) != (0, 0):
                        ship(it, h, k, n, peer, me).wait_send()
        ask(n, peer, me).wait_send()
    for part in range(CUTS):
        for d in range(1, groups):
            bulk(d, part, me).wait_send()
            if cores > 1:
                hand(d, part, origin(d, cores - 1 - core)).wait_send()
    if cores > 1:
        for part in range(CUTS):
            near(part, me).wait_send()
    for n, peer in enumerate(peers):
        share(n, peer, peer).wait_recv()
    every = squares[0]
    for p in range(1, panels):
        every = every + squares[p]
    scale = 1.0 / jnp.sqrt(every / (panels * blk * TILE) + 1e-06)
    for i in range(len(pieces)):
        one = jnp.sum(jnp.where(lane == i, scale, 0.0), axis=1, keepdims=True)
        out_ref[i * 8:(i + 1) * 8, :] = out_ref[i * 8:(i + 1) * 8, :] * one
    for n, peer in enumerate(peers):
        share(n, peer, me).wait_send()


def per_device(tiles, tile_rows, tile_cols, tile_count, seeds, decay):
    slots = tiles.shape[0]
    seed_count = seeds.shape[0]
    blk = seeds.shape[1] // TILE
    panels = lax.axis_size("row")
    width = -(-panels * blk // LANES) * LANES
    square = max(LANES, slots)
    chunks = 8 if slots % 8 == 0 else 1
    halves = HALVES if seed_count % (16 * HALVES) == 0 else 1
    rows = seed_count // halves
    peers = panels - 1
    vmem = pl.BlockSpec(memory_space=pltpu.VMEM)
    return pl.pallas_call(
        functools.partial(kernel, panels, slots, blk, seed_count, chunks, halves),
        out_shape=jax.ShapeDtypeStruct(seeds.shape, jnp.float32),
        in_specs=[pl.BlockSpec(memory_space=pltpu.SMEM)] + [pl.BlockSpec(memory_space=pltpu.HBM)] * 5,
        out_specs=vmem,
        scratch_shapes=[
            pltpu.VMEM((slots, TILE, TILE), jnp.bfloat16),
            pltpu.VMEM((slots, TILE, TILE), jnp.bfloat16),
            pltpu.VMEM(seeds.shape, jnp.float32),
            pltpu.VMEM((halves, CUTS, blk, rows, LANES), jnp.bfloat16),
            pltpu.VMEM((ITERS, halves, CUTS, peers, NEED, rows, LANES), jnp.bfloat16),
            pltpu.VMEM((halves, CUTS, slots, rows, TILE), jnp.float32),
            pltpu.VMEM((8, square), jnp.int32),
            pltpu.VMEM((8, width), jnp.int32),
            pltpu.VMEM((panels, 8, LANES), jnp.float32),
            pltpu.VMEM((1, slots), jnp.int32),
            pltpu.VMEM((1, slots), jnp.int32),
            pltpu.VMEM((1, seed_count), jnp.float32),
            pltpu.SMEM((8, square), jnp.int32),
            pltpu.SMEM((panels, 8, width), jnp.int32),
            *[pltpu.VMEM((panels * blk, rows, LANES), jnp.bfloat16) for _ in range(CUTS)],
            *[
                pltpu.VMEM((panels * NEED, rows, LANES), jnp.bfloat16)
                for _ in range(ITERS * halves * CUTS)
            ],
        ],
        compiler_params=pltpu.CompilerParams(
            collective_id=0, has_side_effects=True, vmem_limit_bytes=53 * 2**20
        ),
    )(tile_count, *[
        pltpu.with_memory_space_constraint(one, pltpu.HBM)
        for one in (
            tile_cols.reshape(1, slots), tile_rows.reshape(1, slots),
            decay.reshape(1, seed_count), seeds, tiles,
        )
    ])


def solution(mesh):
    in_specs = (
        P(("graph", "row"), None, None),
        P(("graph", "row")),
        P(("graph", "row")),
        P(("graph", "row")),
        P(None, ("graph", "row")),
        P(),
    )
    out_specs = P(None, ("graph", "row"))
    return jax.shard_map(
        per_device, mesh=mesh, in_specs=in_specs, out_specs=out_specs, check_vma=False
    )
```

```python
import functools

import jax
import jax.numpy as jnp
from jax import lax
from jax.experimental import pallas as pl
from jax.experimental.pallas import tpu as pltpu
from jax.sharding import PartitionSpec as P

TILE = 256
NEED = 4
HALVES = 2
TAIL = 8
ITERS = 3
MESH = pl.DeviceIdType.MESH
LANES = 128
CUTS = TILE // LANES
ROW_PERM, ROW_PLACE, ROW_KEEP, ROW_LAST, ROW_HAS, ROW_COL = 0, 1, 2, 3, 4, 5


def spread(ref, slots, square):
    wide = jnp.concatenate(
        [ref[...], jnp.zeros((1, square - slots), jnp.int32)], axis=1
    ) if square > slots else ref[...]
    return jnp.broadcast_to(wide, (square, square))


def fill_wanted(cols_ref, count, wanted, slots, blk):
    width = wanted.shape[1]
    square = max(LANES, slots)
    lane = lax.broadcasted_iota(jnp.int32, (square, square), 1)
    col_row = jnp.where((lane < count) & (lane < slots), spread(cols_ref, slots, square), -1)
    col_t = jnp.transpose(col_row)[:slots, :1]
    lane_c = lax.broadcasted_iota(jnp.int32, (slots, width), 1)
    hit = (col_t == lane_c).astype(jnp.int32)
    lane_w = lax.broadcasted_iota(jnp.int32, (8, width), 1)
    local = lane_w % blk
    present = jnp.broadcast_to(jnp.max(hit, axis=0, keepdims=True), (8, width))

    def scan(value):
        step = 1
        while step < blk:
            value = value + jnp.where(local >= step, pltpu.roll(value, step, 1), 0)
            step *= 2
        return value

    rank = scan(present) - 1
    which = lax.broadcasted_iota(jnp.int32, (8, width), 0)
    chosen = (present > 0) & (rank == which)
    wanted[...] = scan(jnp.where(chosen, local, 0))
    weight = (lane_w // blk) * NEED + rank
    return hit, weight, col_t


def fill_own(rows_ref, count, own_table, hit, weight, col_t, slots, blk):
    width = hit.shape[1]
    square = max(LANES, slots)
    lane = lax.broadcasted_iota(jnp.int32, (square, square), 1)
    sub = lax.broadcasted_iota(jnp.int32, (square, square), 0)
    key_row = jnp.where(lane < count, spread(rows_ref, slots, square), blk)
    key_row = jnp.where(lane < slots, key_row, blk + 1)
    key_c = jnp.transpose(key_row)[:slots, :]
    key_r = key_row[:slots, :]
    place_col = jnp.sum(hit * weight[:1, :], axis=1, keepdims=True)
    place_col = jnp.clip(place_col, 0, (width // blk) * NEED - 1)
    lane_s, sub_s = lane[:slots, :], sub[:slots, :]
    before = (key_r < key_c) | ((key_r == key_c) & (lane_s < sub_s))
    position = jnp.sum((before & (lane_s < slots)).astype(jnp.int32), axis=1, keepdims=True)
    at = position == lane_s
    perm = jnp.sum(jnp.where(at, sub_s, 0), axis=0, keepdims=True)
    place = jnp.sum(jnp.where(at, place_col, 0), axis=0, keepdims=True)
    column = jnp.sum(jnp.where(at, jnp.clip(col_t, 0, width - 1), 0), axis=0, keepdims=True)
    key_sorted = jnp.sum(jnp.where(at, key_c, 0), axis=0, keepdims=True)
    previous = jnp.sum(jnp.where(position + 1 == lane_s, key_c, 0), axis=0, keepdims=True)
    keep = ((key_sorted == previous) & (lane_s[:1, :] > 0)).astype(jnp.int32)
    last = jnp.sum((key_c <= lane_s).astype(jnp.int32), axis=0, keepdims=True) - 1
    has = jnp.max((key_c == lane_s).astype(jnp.int32), axis=0, keepdims=True)
    own_table[...] = jnp.zeros(own_table.shape, jnp.int32)
    own_table[ROW_PERM:ROW_PERM + 1, :] = perm
    own_table[ROW_PLACE:ROW_PLACE + 1, :] = place
    own_table[ROW_KEEP:ROW_KEEP + 1, :] = keep
    own_table[ROW_LAST:ROW_LAST + 1, :] = jnp.maximum(last, 0)
    own_table[ROW_HAS:ROW_HAS + 1, :] = has
    own_table[ROW_COL:ROW_COL + 1, :] = column


def kernel(
    panels, slots, blk, seed_count, chunks, halves,
    count_ref, cols_hbm, rows_hbm, decay_hbm, seeds_hbm, tiles_hbm,
    out_ref,
    tiles, turned, seeds_ref, current, outgoing, partial, own_table, wanted, squares,
    rows_ref, cols_ref, decay_ref, own_s, wanted_s,
    *landing,
):
    whole, arrivals = landing[:CUTS], landing[CUTS:]
    dma = pltpu.SemaphoreType.DMA
    peers, far = panels - 1, max(panels // (2 if panels % 2 == 0 else 1) - 1, 1)
    pl.run_scoped(
        functools.partial(
            body, panels, slots, blk, seed_count, chunks, halves,
            count_ref, cols_hbm, rows_hbm, decay_hbm, seeds_hbm, tiles_hbm,
            out_ref,
            tiles, turned, seeds_ref, current, outgoing, partial, own_table, wanted, squares,
            rows_ref, cols_ref, decay_ref, own_s, wanted_s, whole, arrivals,
        ),
        dma((chunks,)), dma((halves,)), dma((3,)), dma((2,)), dma((peers,)), dma((panels,)),
        dma((ITERS, halves, CUTS, peers)), dma((ITERS, halves, CUTS, panels)), dma((peers,)), dma((panels,)),
        dma((far, CUTS)), dma((far, CUTS)), dma((far, CUTS)), dma((far, CUTS)), dma((CUTS,)), dma((CUTS,)),
    )


def body(
    panels, slots, blk, seed_count, chunks, halves,
    count_ref, cols_hbm, rows_hbm, decay_hbm, seeds_hbm, tiles_hbm,
    out_ref,
    tiles, turned, seeds_ref, current, outgoing, partial, own_table, wanted, squares,
    rows_ref, cols_ref, decay_ref, own_s, wanted_s, whole, arrivals,
    tile_sem, seed_sem, small_sem, table_sem,
    want_send, want_recv, send_sem, recv_sem, norm_send, norm_recv,
    bulk_send, bulk_recv, pass_send, pass_recv, near_send, near_recv,
):
    me = lax.axis_index("row")
    cores = 2 if panels % 2 == 0 else 1
    chip, core = me // cores, me % cores
    groups = panels // cores
    rows = seed_count // halves
    peers = [
        lax.rem(chip + d, groups) * cores + e
        for d in range(groups - 1, 0, -1) for e in range(cores)
    ] + [chip * cores + lax.rem(core + e, cores) for e in range(1, cores)]
    away = (groups - 1) * cores

    small = [
        pltpu.make_async_copy(src, dst, small_sem.at[n])
        for n, (src, dst) in enumerate([
            (cols_hbm, cols_ref), (rows_hbm, rows_ref), (decay_hbm, decay_ref),
        ])
    ]
    for copy in small:
        copy.start()
    barrier = pltpu.get_barrier_semaphore()
    for peer in peers:
        pl.semaphore_signal(barrier, inc=1, device_id={"row": peer}, device_id_type=MESH)

    def seed_load(h):
        mine = pl.ds(h * rows, rows)
        return pltpu.make_async_copy(seeds_hbm.at[mine], seeds_ref.at[mine], seed_sem.at[h])

    for h in range(halves):
        seed_load(h).start()
    per = slots // chunks

    def load(c):
        return pltpu.make_async_copy(
            tiles_hbm.at[pl.ds(c * per, per)], tiles.at[pl.ds(c * per, per)], tile_sem.at[c]
        )

    for c in range(chunks):
        load(c).start(priority=1)

    small[0].wait()
    count = count_ref[0]
    hit, weight, col_t = fill_wanted(cols_ref, count, wanted, slots, blk)
    seed_load(0).wait()
    def convert(k):
        for b in range(blk):
            nodes = slice(b * TILE + k * LANES, b * TILE + (k + 1) * LANES)
            whole[k][me * blk + b] = seeds_ref[:rows, nodes].astype(jnp.bfloat16)

    convert(0)
    pl.semaphore_wait(barrier, panels - 1)

    def ask(n, peer, source):
        return pltpu.make_async_remote_copy(
            src_ref=wanted.at[pl.ds(0, NEED)], dst_ref=wanted_s.at[source, pl.ds(0, NEED)],
            send_sem=want_send.at[n], recv_sem=want_recv.at[source],
            device_id={"row": peer}, device_id_type=MESH,
        )

    for n, peer in enumerate(peers):
        ask(n, peer, me).start()
    partner = chip * cores + (cores - 1 - core)

    def block(source, part):
        return whole[part].at[pl.ds(source * blk, blk)]

    def bulk(d, part, source):
        far = lax.rem(chip + d, groups) * cores + (cores - 1 - core)
        return pltpu.make_async_remote_copy(
            src_ref=block(source, part), dst_ref=block(source, part),
            send_sem=bulk_send.at[d - 1, part], recv_sem=bulk_recv.at[d - 1, part],
            device_id={"row": far}, device_id_type=MESH,
        )

    def hand(d, part, source):
        return pltpu.make_async_remote_copy(
            src_ref=block(source, part), dst_ref=block(source, part),
            send_sem=pass_send.at[d - 1, part], recv_sem=pass_recv.at[d - 1, part],
            device_id={"row": partner}, device_id_type=MESH,
        )

    def near(part, source):
        return pltpu.make_async_remote_copy(
            src_ref=block(source, part), dst_ref=block(source, part),
            send_sem=near_send.at[part], recv_sem=near_recv.at[part],
            device_id={"row": partner}, device_id_type=MESH,
        )

    def origin(d, index):
        return lax.rem(chip + groups - d, groups) * cores + index

    for part in range(CUTS):
        if part > 0:
            convert(part)
        for d in range(1, groups):
            bulk(d, part, me).start()
    if cores > 1:
        for part in range(CUTS):
            near(part, me).start()
    want_copy = pltpu.make_async_copy(wanted, wanted_s.at[me], table_sem.at[1])
    want_copy.start()
    small[1].wait()
    fill_own(rows_ref, count, own_table, hit, weight, col_t, slots, blk)
    own_copy = pltpu.make_async_copy(own_table, own_s, table_sem.at[0])
    own_copy.start()
    small[2].wait()
    for h in range(1, halves):
        seed_load(h).wait()
        for b in range(blk):
            for k in range(CUTS):
                current[h, k, b] = seeds_ref[
                    h * rows:(h + 1) * rows, b * TILE + k * LANES:b * TILE + (k + 1) * LANES
                ].astype(jnp.bfloat16)
    diagonal = lax.broadcasted_iota(jnp.int32, (seed_count, seed_count), 0) == (
        lax.broadcasted_iota(jnp.int32, (seed_count, seed_count), 1)
    )
    decay = jnp.sum(
        jnp.where(diagonal, jnp.broadcast_to(decay_ref[...], diagonal.shape), 0.0),
        axis=1, keepdims=True,
    )

    def turn(c, carry):
        load(c).wait()
        for i in range(per):
            turned[c * per + i] = jnp.transpose(tiles[c * per + i])
        return carry

    early = chunks * 8 // 8
    lax.fori_loop(0, early, turn, 0)
    for n, peer in enumerate(peers):
        ask(n, peer, peer).wait_recv()
    want_copy.wait()

    def ship(it, h, k, n, peer, source):
        return pltpu.make_async_remote_copy(
            src_ref=outgoing.at[it, h, k, n],
            dst_ref=arrivals[(it * halves + h) * CUTS + k].at[pl.ds(source * NEED, NEED)],
            send_sem=send_sem.at[it, h, k, n], recv_sem=recv_sem.at[it, h, k, source],
            device_id={"row": peer}, device_id_type=MESH,
        )

    def exchange(it, h, k):
        arrived = arrivals[(it * halves + h) * CUTS + k]
        last = k == CUTS - 1
        for n, peer in enumerate(peers[:away]):
            for w in range(NEED):
                outgoing[it, h, k, n, w] = current[h, k, wanted_s[peer, w, me * blk + blk - 1]]
            ship(it, h, k, n, peer, me).start()
        for c in range(CUTS) if last else ():
            for n, peer in list(enumerate(peers))[away:]:
                for w in range(NEED):
                    outgoing[it, h, c, n, w] = current[h, c, wanted_s[peer, w, me * blk + blk - 1]]
                ship(it, h, c, n, peer, me).start()
        for w in range(NEED):
            arrived[me * NEED + w] = current[h, k, wanted_s[me, w, me * blk + blk - 1]]

    for h in range(1, halves):
        for k in range(CUTS):
            exchange(0, h, k)
    lax.fori_loop(early, chunks, turn, 0)
    for part in range(CUTS):
        for d in range(1, groups):
            source = origin(d, cores - 1 - core)
            bulk(d, part, source).wait_recv()
            if cores > 1:
                hand(d, part, source).start()

    own_copy.wait()

    totals = []
    for it in range(ITERS):
        for h in range(halves):
            first = it == 0 and h == 0
            def contract(arrived, place, k, nodes, some, acc):
                for j in some:
                    product = jnp.dot(
                        arrived[own_s[place, j]],
                        turned[own_s[ROW_PERM, j], nodes, :],
                        preferred_element_type=jnp.float32,
                    )
                    acc = acc * own_s[ROW_KEEP, j].astype(jnp.float32) + product
                    partial[h, k, j] = acc
                return acc

            zero = jnp.zeros((rows, TILE), jnp.float32)
            def arrive(k):
                if not first:
                    for n, peer in enumerate(peers):
                        ship(it, h, k, n, peer, peer).wait_recv()
                elif cores > 1:
                    near(k, partner).wait_recv()
                    for d in range(1, groups):
                        hand(d, k, origin(d, core)).wait_recv()

            rest = range(0)
            for k in range(CUTS):
                arrive(k)
                if k > 0:
                    contract(*use, rest, acc)
                use = (
                    whole[k] if first else arrivals[(it * halves + h) * CUTS + k],
                    ROW_COL if first else ROW_PLACE, k, slice(k * LANES, (k + 1) * LANES),
                )
                cut = slots - TAIL if k < CUTS - 1 else slots
                acc = contract(*use, range(cut), zero)
                rest = range(cut, slots)

            mine = slice(h * rows, (h + 1) * rows)
            total = jnp.zeros((rows, LANES), jnp.float32)
            for k in range(CUTS):
                out = slice(k * LANES, (k + 1) * LANES)
                for r in range(blk):
                    last = own_s[ROW_LAST, r]
                    summed = partial[h, 0, last, :, out]
                    for c in range(1, CUTS):
                        summed = summed + partial[h, c, last, :, out]
                    summed = summed * own_s[ROW_HAS, r].astype(jnp.float32)
                    nodes = slice(r * TILE + k * LANES, r * TILE + (k + 1) * LANES)
                    value = decay[mine] * summed + seeds_ref[mine, nodes]
                    if it < ITERS - 1:
                        current[h, k, r] = value.astype(jnp.bfloat16)
                    else:
                        out_ref[mine, nodes] = value
                        total = total + value * value
                if it < ITERS - 1:
                    exchange(it + 1, h, k)
            if it == ITERS - 1:
                totals.append(jnp.sum(total, axis=1, keepdims=True))

    lane = lax.broadcasted_iota(jnp.int32, (8, LANES), 1)
    packed = jnp.zeros((8, LANES), jnp.float32)
    pieces = [t[i:i + 8] for t in totals for i in range(0, rows, 8)]
    for i, piece in enumerate(pieces):
        packed = jnp.where(lane == i, piece, packed)
    squares[me] = packed

    def share(n, peer, source):
        return pltpu.make_async_remote_copy(
            src_ref=squares.at[me], dst_ref=squares.at[source],
            send_sem=norm_send.at[n], recv_sem=norm_recv.at[source],
            device_id={"row": peer}, device_id_type=MESH,
        )

    for n, peer in enumerate(peers):
        share(n, peer, me).start()
    for n, peer in enumerate(peers):
        for it in range(ITERS):
            for h in range(halves):
                for k in range(CUTS):
                    if (it, h) != (0, 0):
                        ship(it, h, k, n, peer, me).wait_send()
        ask(n, peer, me).wait_send()
    for part in range(CUTS):
        for d in range(1, groups):
            bulk(d, part, me).wait_send()
            if cores > 1:
                hand(d, part, origin(d, cores - 1 - core)).wait_send()
    if cores > 1:
        for part in range(CUTS):
            near(part, me).wait_send()
    for n, peer in enumerate(peers):
        share(n, peer, peer).wait_recv()
    every = squares[0]
    for p in range(1, panels):
        every = every + squares[p]
    scale = lax.rsqrt(every / (panels * blk * TILE) + 1e-06)
    for i in range(len(pieces)):
        one = jnp.sum(jnp.where(lane == i, scale, 0.0), axis=1, keepdims=True)
        out_ref[i * 8:(i + 1) * 8, :] = out_ref[i * 8:(i + 1) * 8, :] * one
    for n, peer in enumerate(peers):
        share(n, peer, me).wait_send()


def per_device(tiles, tile_rows, tile_cols, tile_count, seeds, decay):
    slots = tiles.shape[0]
    seed_count = seeds.shape[0]
    blk = seeds.shape[1] // TILE
    panels = lax.axis_size("row")
    width = -(-panels * blk // LANES) * LANES
    square = max(LANES, slots)
    chunks = 8 if slots % 8 == 0 else 1
    halves = HALVES if seed_count % (16 * HALVES) == 0 else 1
    rows = seed_count // halves
    peers = panels - 1
    vmem = pl.BlockSpec(memory_space=pltpu.VMEM)
    return pl.pallas_call(
        functools.partial(kernel, panels, slots, blk, seed_count, chunks, halves),
        out_shape=jax.ShapeDtypeStruct(seeds.shape, jnp.float32),
        in_specs=[pl.BlockSpec(memory_space=pltpu.SMEM)] + [pl.BlockSpec(memory_space=pltpu.HBM)] * 5,
        out_specs=vmem,
        scratch_shapes=[
            pltpu.VMEM((slots, TILE, TILE), jnp.bfloat16),
            pltpu.VMEM((slots, TILE, TILE), jnp.bfloat16),
            pltpu.VMEM(seeds.shape, jnp.float32),
            pltpu.VMEM((halves, CUTS, blk, rows, LANES), jnp.bfloat16),
            pltpu.VMEM((ITERS, halves, CUTS, peers, NEED, rows, LANES), jnp.bfloat16),
            pltpu.VMEM((halves, CUTS, slots, rows, TILE), jnp.float32),
            pltpu.VMEM((8, square), jnp.int32),
            pltpu.VMEM((8, width), jnp.int32),
            pltpu.VMEM((panels, 8, LANES), jnp.float32),
            pltpu.VMEM((1, slots), jnp.int32),
            pltpu.VMEM((1, slots), jnp.int32),
            pltpu.VMEM((1, seed_count), jnp.float32),
            pltpu.SMEM((8, square), jnp.int32),
            pltpu.SMEM((panels, 8, width), jnp.int32),
            *[pltpu.VMEM((panels * blk, rows, LANES), jnp.bfloat16) for _ in range(CUTS)],
            *[
                pltpu.VMEM((panels * NEED, rows, LANES), jnp.bfloat16)
                for _ in range(ITERS * halves * CUTS)
            ],
        ],
        compiler_params=pltpu.CompilerParams(
            collective_id=0, has_side_effects=True, vmem_limit_bytes=53 * 2**20
        ),
    )(tile_count, *[
        pltpu.with_memory_space_constraint(one, pltpu.HBM)
        for one in (
            tile_cols.reshape(1, slots), tile_rows.reshape(1, slots),
            decay.reshape(1, seed_count), seeds, tiles,
        )
    ])


def solution(mesh):
    in_specs = (
        P(("graph", "row"), None, None),
        P(("graph", "row")),
        P(("graph", "row")),
        P(("graph", "row")),
        P(None, ("graph", "row")),
        P(),
    )
    out_specs = P(None, ("graph", "row"))
    return jax.shard_map(
        per_device, mesh=mesh, in_specs=in_specs, out_specs=out_specs, check_vma=False
    )
```
